512 devices in a mesh: gx: 8 (over y, core), gy: 8 (over z_lo), gz: 8 (over x, z_hi).
Axes of the slice: x: 4, y: 4, z: 16 (z_hi: 2, z_lo: 8; z = z_hi * 8 + z_lo), core: 2. Of those that a mesh axis runs over, the one named last changes fastest.
Arguments:
- positions: float32 [3, 16, 16, 16, 256], P(None, 'gx', 'gy', 'gz'), may hold values from 0 to 1
- velocities: float32 [3, 16, 16, 16, 256], P(None, 'gx', 'gy', 'gz'), may hold values from -3 to 3
- masses: float32 [16, 16, 16, 256], P('gx', 'gy', 'gz'), may hold values from 0.0025 to 0.01
- entropy: float32 [16, 16, 16, 256], P('gx', 'gy', 'gz'), may hold values from 0.5 to 2
- counts: int32 [16, 16, 16], P('gx', 'gy', 'gz'), may hold values from 8 to 256, as said below
Outputs:
- density: float32 [16, 16, 16, 256], P('gx', 'gy', 'gz')
- acceleration: float32 [3, 16, 16, 16, 256], P(None, 'gx', 'gy', 'gz')
The draws below stay inside these ranges and needn't reach their ends.
Inputs may be any that keep to these rules, and one draw needn't show every extreme that they name: The first counts[c] slots of cell c hold particles; the other slots of the cell are padding whose values are arbitrary.
All inputs are finite; a program needn't handle non-finite values.
Results may differ from the reference program's by a relative error of at most 0.0003.
Values sent between devices are 32-bit elements; how exact they have to be, the bound alone decides.
A program may use at most 64 MiB of HBM per device.

```python
import math
import jax
import jax.numpy as jnp
from jax import lax

LX = 2
LY = 2
LZ = 2
PC = 256
NX = 16
NY = 16
NZ = 16
N_GX = 8
N_GY = 8
N_GZ = 8


def draw_counts(key, part):
    key_base, key_crowd, key_rare, key_half = jax.random.split(key, 4)
    base_count = jax.random.randint(key_base, (NX, NY, NZ), 8, PC // 2 + 1)
    crowded = jax.random.randint(key_crowd, (NX // LX, NY // LY, NZ // LZ), 0, 6) == 0
    crowded = jnp.repeat(jnp.repeat(jnp.repeat(crowded, LX, 0), LY, 1), LZ, 2)
    rare_full = jax.random.randint(key_rare, (NX, NY, NZ), 0, 64) == 0
    half_full = jax.random.randint(key_half, (NX, NY, NZ), 0, 2) == 0
    heavy = rare_full | crowded & half_full
    heavy = heavy.at[0, 0, 0].set(True)
    return jnp.where(heavy, PC, base_count).astype(jnp.int32)


def steps_of(rng, shape, cuts, least, top_value):
    gain, own = 1.0, jax.random.fold_in(rng, 6)
    for dim, parts in cuts:
        steps = jnp.exp(jax.random.uniform(jax.random.fold_in(own, dim), (parts,), jnp.float32, least / len(cuts), top_value / len(cuts)))
        gain = gain * jnp.repeat(steps, shape[dim] // parts).reshape([-1 if axis == dim else 1 for axis in range(len(shape))])
    return gain


def normal_values(own_key, extent, width, most, shards=(), kind=jnp.bfloat16):
    array = width * jax.random.normal(own_key, extent, jnp.float32)
    if shards:
        array = array * steps_of(own_key, extent, shards, -0.22, 0.18)
    return jnp.clip(array, -most, most).astype(kind)


def setup_inputs(seed: int = 0) -> dict:
    seeds = jax.random.split(jax.random.key(seed), 6)
    positions = jnp.clip(1.0 * jax.random.uniform(seeds[0], (3, NX, NY, NZ, PC), jnp.float32) ** steps_of(seeds[0], (3, NX, NY, NZ, PC), ((1, 8), (2, 8), (3, 8)), -0.2, 0.2), 0.0, 1.0)
    velocities = normal_values(seeds[1], (3, NX, NY, NZ, PC), 0.5, 3.0, ((1, 8), (2, 8), (3, 8)), jnp.float32)
    masses = jnp.clip(jnp.exp(math.log(0.01) - 1.3862944 * jax.random.uniform(seeds[2], (NX, NY, NZ, PC), jnp.float32) ** steps_of(seeds[2], (NX, NY, NZ, PC), ((0, 8), (1, 8), (2, 8)), -0.2, 0.2)), 0.0025, 0.01)
    entropy = jnp.clip(jnp.exp(math.log(2.0) - 1.3862944 * jax.random.uniform(seeds[3], (NX, NY, NZ, PC), jnp.float32) ** steps_of(seeds[3], (NX, NY, NZ, PC), ((0, 8), (1, 8), (2, 8)), -0.2, 0.2)), 0.5, 2.0)
    counts = draw_counts(jax.random.fold_in(seeds[5], 71), 0)
    return dict(positions=positions, velocities=velocities, masses=masses, entropy=entropy, counts=counts)


SIGMA = 8.0 / math.pi
GAMMA = 5.0 / 3.0
ALPHA = 1.0
BETA = 2.0
SOFTEN = 0.01

def kernel_value(radius_sq):
    radius = jnp.sqrt(radius_sq)
    near_part = 1.0 - 6.0 * radius * radius + 6.0 * radius * radius * radius
    far_part = 2.0 * (1.0 - radius) ** 3
    return SIGMA * jnp.where(radius < 0.5, near_part, jnp.where(radius < 1.0, far_part, 0.0))

def kernel_slope(radius_sq):
    radius = jnp.sqrt(radius_sq)
    near_part = -12.0 + 18.0 * radius
    far_part = -6.0 * (1.0 - radius) ** 2 / jnp.maximum(radius, 0.5)
    return SIGMA * jnp.where(radius < 0.5, near_part, jnp.where(radius < 1.0, far_part, 0.0))

def block_of(values, start_x, start_y, start_z, size_x, size_y, size_z):
    leading = values.shape[:-4]
    anchor = jnp.zeros((), jnp.int32)
    starts = (anchor,) * len(leading) + (start_x, start_y, start_z, anchor)
    return lax.dynamic_slice(values, starts, leading + (size_x, size_y, size_z, values.shape[-1]))

def flatten(values):
    return values.reshape(values.shape[:-4] + (-1, values.shape[-1]))

def offsets(number):
    number = jnp.asarray(number).astype(jnp.int32)
    return (number // 9, number // 3 % 3, number % 3)

def density_sum(targets, grid_pos, grid_weight, rows):
    size_x, size_y, size_z = (grid_pos.shape[1] - 2, grid_pos.shape[2] - 2, grid_pos.shape[3] - 2)
    picked = jnp.moveaxis(targets[:, :, :rows], 1, 0)

    def add_cells(number, running):
        step_x, step_y, step_z = offsets(number)
        source = jnp.moveaxis(flatten(block_of(grid_pos, step_x, step_y, step_z, size_x, size_y, size_z)), 1, 0)
        source_weight = flatten(block_of(grid_weight, step_x, step_y, step_z, size_x, size_y, size_z))
        displace = jnp.stack([step_x, step_y, step_z]).astype(jnp.float32) - 1.0

        def one_cell(items):
            own, far, far_weight = items
            between = own[:, :, None] - far[:, None, :] - displace[:, None, None]
            radius_sq = lax.optimization_barrier(jnp.sum(between * between, 0))
            return lax.optimization_barrier(jnp.sum(far_weight[None, :] * kernel_value(radius_sq), 1))
        return running + lax.map(one_cell, (picked, source, source_weight))
    return lax.fori_loop(0, 27, add_cells, jnp.zeros((picked.shape[0], picked.shape[2]), jnp.float32))

def force_sum(targets, margins, rows):
    own_pos, own_vel, own_rho, own_sound, own_press = [item[..., :rows] for item in targets]
    own_pos = jnp.moveaxis(own_pos, 1, 0)
    own_vel = jnp.moveaxis(own_vel, 1, 0)
    size_x, size_y, size_z = (margins[0].shape[1] - 2, margins[0].shape[2] - 2, margins[0].shape[3] - 2)

    def add_cells(number, running):
        step_x, step_y, step_z = offsets(number)
        pieces = [flatten(block_of(item, step_x, step_y, step_z, size_x, size_y, size_z)) for item in margins]
        far_pos, far_vel, far_weight, far_rho, far_sound, far_press = pieces
        far_pos = jnp.moveaxis(far_pos, 1, 0)
        far_vel = jnp.moveaxis(far_vel, 1, 0)
        displace = jnp.stack([step_x, step_y, step_z]).astype(jnp.float32) - 1.0

        def one_cell(items):
            mine_pos, mine_vel, mine_rho, mine_sound, mine_press, other_pos, other_vel, other_weight, other_rho, other_sound, other_press = items
            between = mine_pos[:, :, None] - other_pos[:, None, :] - displace[:, None, None]
            radius_sq = lax.optimization_barrier(jnp.sum(between * between, 0))
            closing = lax.optimization_barrier(jnp.sum((mine_vel[:, :, None] - other_vel[:, None, :]) * between, 0))
            approach = jnp.minimum(closing, 0.0) / (radius_sq + SOFTEN)
            mean_sound = 0.5 * (mine_sound[:, None] + other_sound[None, :])
            mean_rho = 0.5 * (mine_rho[:, None] + other_rho[None, :])
            viscous = (BETA * approach * approach - ALPHA * mean_sound * approach) / mean_rho
            factor = other_weight[None, :] * (mine_press[:, None] + other_press[None, :] + viscous) * kernel_slope(radius_sq)
            return lax.optimization_barrier(jnp.sum(factor[None] * between, 2))
        items = (own_pos, own_vel, own_rho, own_sound, own_press, far_pos, far_vel, far_weight, far_rho, far_sound, far_press)
        return running - lax.map(one_cell, items)
    total = lax.fori_loop(0, 27, add_cells, jnp.zeros(own_pos.shape, jnp.float32))
    return jnp.moveaxis(total, 0, 1)

def states_of(safe_density, entropy):
    pressure_term = entropy * safe_density ** (GAMMA - 2.0)
    sound_speed = jnp.sqrt(GAMMA * entropy * safe_density ** (GAMMA - 1.0))
    return (pressure_term, sound_speed)

def periodic(values):
    widths = [(0, 0)] * (values.ndim - 4) + [(1, 1)] * 3 + [(0, 0)]
    return jnp.pad(values, widths, mode='wrap')

def assemble(blocks):
    leading = blocks.shape[1:-2]
    lead_count = len(leading)
    shaped = blocks.reshape((N_GX, N_GY, N_GZ) + leading + (LX, LY, LZ, PC))
    reorder = tuple(range(3, 3 + lead_count)) + (0, 3 + lead_count, 1, 4 + lead_count, 2, 5 + lead_count, 6 + lead_count)
    return shaped.transpose(reorder).reshape(leading + (NX, NY, NZ, PC))

def corners(number):
    along_x = number // (N_GY * N_GZ)
    along_y = number // N_GZ % N_GY
    along_z = number % N_GZ
    return (along_x * LX, along_y * LY, along_z * LZ)

def reference(positions, velocities, masses, entropy, counts):
    slot_ids = lax.broadcasted_iota(jnp.int32, masses.shape, 3)
    active = slot_ids < counts[..., None]
    weight = jnp.where(active, masses, 0.0)
    wide_pos = periodic(positions)
    wide_weight = periodic(weight)
    numbers = jnp.arange(N_GX * N_GY * N_GZ, dtype=jnp.int32)

    def block_density(number):
        corner_x, corner_y, corner_z = corners(number)
        targets = flatten(block_of(positions, corner_x, corner_y, corner_z, LX, LY, LZ))
        grid_pos = block_of(wide_pos, corner_x, corner_y, corner_z, LX + 2, LY + 2, LZ + 2)
        grid_weight = block_of(wide_weight, corner_x, corner_y, corner_z, LX + 2, LY + 2, LZ + 2)
        return density_sum(targets, grid_pos, grid_weight, PC)
    raw_density = assemble(lax.map(block_density, numbers))
    safe_density = jnp.where(active, raw_density, 1.0)
    pressure_term, sound_speed = states_of(safe_density, entropy)
    owned = (positions, velocities, safe_density, sound_speed, pressure_term)
    widened = [periodic(item) for item in (positions, velocities, weight, safe_density, sound_speed, pressure_term)]

    def block_force(number):
        corner_x, corner_y, corner_z = corners(number)
        targets = tuple((flatten(block_of(item, corner_x, corner_y, corner_z, LX, LY, LZ)) for item in owned))
        margins = tuple((block_of(item, corner_x, corner_y, corner_z, LX + 2, LY + 2, LZ + 2) for item in widened))
        return force_sum(targets, margins, PC)
    raw_accel = assemble(lax.map(block_force, numbers))
    density = jnp.where(active, raw_density, 0.0)
    acceleration = jnp.where(active[None], raw_accel, 0.0)
    return (density, acceleration)
```

```python
import functools
import math

import jax
import jax.numpy as jnp
from jax import lax
from jax.experimental import pallas as pl
from jax.experimental.pallas import tpu as pltpu
from jax.sharding import PartitionSpec as P

SIGMA = 8.0 / math.pi
GAMMA = 5.0 / 3.0
SOFTEN = 0.01
TINY = 1e-12
SLOTS = 256
WIDE = 4
CELLS = WIDE * WIDE * WIDE
OWN = 8
LANES = 128
TILES = 2 * CELLS
EMPTY = TILES
UNROLL = 4
LIST = 64
MAX_STEPS = 2 * OWN * 14 + 8
FIELDS = 8
F32 = jnp.float32
BF16 = jnp.bfloat16


def cell_id(x, y, z):
    return (x * WIDE + y) * WIDE + z


def own_cells():
    return [cell_id(1 + n // 4, 1 + n // 2 % 2, 1 + n % 2) for n in range(OWN)]


def neighbours(number):
    x, y, z = 1 + number // 4, 1 + number // 2 % 2, 1 + number % 2
    return [
        cell_id(x + dx, y + dy, z + dz)
        for dx in (-1, 0, 1)
        for dy in (-1, 0, 1)
        for dz in (-1, 0, 1)
    ]


def build_lists(full_ref, tiles, first, chunk_of):
    def add_steps(total, number, chunk, count):
        def put(index, total):
            first[total] = number * LIST + index * UNROLL
            chunk_of[total] = chunk
            return total + 1

        return lax.fori_loop(0, count, put, total)

    total = jnp.int32(0)
    for number, own in enumerate(own_cells()):
        where = jnp.int32(number * LIST)
        for other in neighbours(number):
            tiles[where] = jnp.int32(2 * other)
            tiles[where + 1] = jnp.int32(2 * other + 1)
            where = where + 1 + full_ref[other]
        for extra in range(UNROLL - 1):
            tiles[where + extra] = jnp.int32(EMPTY)
        count = (where - number * LIST + UNROLL - 1) // UNROLL
        total = add_steps(total, number, jnp.int32(2 * number), count)
        total = add_steps(total, number, jnp.int32(2 * number + 1), count * full_ref[own])
    for extra in range(UNROLL):
        tiles[OWN * LIST + extra] = jnp.int32(EMPTY)
    for extra in range(3):
        first[total + extra] = jnp.int32(OWN * LIST)
        chunk_of[total + extra] = jnp.int32(2 * OWN)
    return total


def split(value):
    high = value.astype(BF16).astype(F32)
    rest = value - high
    middle = rest.astype(BF16).astype(F32)
    low = rest - middle
    return high, middle, low


def field_of(h_ref, number):
    return h_ref[pl.ds(number, TILES, stride=FIELDS), :]


def cell_axes():
    ids = lax.broadcasted_iota(jnp.int32, (TILES, LANES), 0) // 2
    axes = (ids // (WIDE * WIDE), ids // WIDE % WIDE, ids % WIDE)
    return [axis.astype(F32) - 2.0 for axis in axes]


def put_rows(ref, rows, width):
    for number, value in enumerate(rows):
        ref[pl.ds(number, TILES, stride=width), :] = value


PAIRS = ((0, 0), (0, 1), (1, 0), (1, 1), (0, 2), (2, 0))


def density_kernel(full_ref, h_ref, out_ref, source, target, source16, target16, weights, far0, far1, total_acc, tiles, first, chunk_of):
    steps = build_lists(full_ref, tiles, first, chunk_of)
    weight = field_of(h_ref, 3)
    active = weight > 0.0
    places = [
        jnp.where(active, field_of(h_ref, axis) + base, 0.0)
        for axis, base in enumerate(cell_axes())
    ]
    norm = split(places[0] * places[0] + places[1] * places[1] + places[2] * places[2])
    one = jnp.ones_like(weight)
    zero = jnp.zeros_like(weight)
    source_rows, target_rows = [], []
    for place in places:
        pieces = split(place)
        for mine, theirs in PAIRS:
            target_rows.append(-2.0 * pieces[mine])
            source_rows.append(pieces[theirs])
    for piece in norm:
        target_rows.append(one)
        source_rows.append(piece)
    for piece in norm:
        target_rows.append(piece)
        source_rows.append(one)
    width = 32
    while len(source_rows) < width:
        target_rows.append(zero)
        source_rows.append(zero)
    put_rows(source, source_rows, width)
    put_rows(target, target_rows, width)

    def convert(pair, carry):
        for half in range(2):
            tile = 2 * pair + half
            source16[tile] = source[pl.ds(pl.multiple_of(tile * width, width), width), :].astype(BF16)
            weights[tile] = h_ref[pl.ds(pl.multiple_of(tile * FIELDS, FIELDS), FIELDS), :]
        return carry

    lax.fori_loop(0, CELLS, convert, 0)
    source16[EMPTY] = jnp.zeros((width, LANES), BF16)
    weights[EMPTY] = jnp.zeros((FIELDS, LANES), F32)
    for number, own in enumerate(own_cells()):
        for half in range(2):
            tile = 2 * own + half
            block = target[tile * width : (tile + 1) * width, :]
            target16[2 * number + half] = block.T.astype(BF16)
    target16[2 * OWN] = jnp.zeros((LANES, width), BF16)
    total_acc[...] = jnp.zeros_like(total_acc)

    def distances(step, far):
        mine = target16[chunk_of[step]]
        start = first[step]
        for pair in range(UNROLL // 2):
            both = jnp.concatenate(
                [source16[tiles[start + 2 * pair]], source16[tiles[start + 2 * pair + 1]]], axis=1
            )
            far[pair] = jnp.dot(mine, both, preferred_element_type=F32)

    def add(step, far):
        chunk = chunk_of[step]
        start = first[step]
        mass = [weights[tiles[start + number], 3:4, :] for number in range(UNROLL)]
        for group in range(LANES // 8):
            rows = slice(group * 8, group * 8 + 8)
            acc = total_acc[chunk, rows, :]
            for number in range(UNROLL):
                lanes = slice((number % 2) * LANES, (number % 2 + 1) * LANES)
                square = jnp.maximum(far[number // 2, rows, lanes], TINY)
                radius = square * lax.rsqrt(square)
                rest = 1.0 - radius
                near = 0.5 - 3.0 * (square * rest)
                clipped = jnp.maximum(rest, 0.0)
                value = jnp.minimum(near, clipped * clipped * clipped)
                acc = acc + value * mass[number]
            total_acc[chunk, rows, :] = acc

    distances(0, far0)

    def two_steps(pair, carry):
        step = 2 * pair
        distances(step + 1, far1)
        add(step, far0)
        distances(step + 2, far0)
        add(step + 1, far1)
        return carry

    lax.fori_loop(0, (steps + 1) // 2, two_steps, 0)
    for number in range(OWN):
        for half in range(2):
            folded = total_acc[2 * number + half].T
            out_ref[number : number + 1, half * LANES : (half + 1) * LANES] = (
                2.0 * SIGMA
            ) * jnp.sum(folded, axis=0, keepdims=True)


def force_kernel(full_ref, h_ref, rho_ref, out_ref, source, target, extra, gather, source16, target16, fields, gather16, mine_c, mine_r, mine_p, far0, far1, force0, force1, total_acc, tiles, first, chunk_of):
    steps = build_lists(full_ref, tiles, first, chunk_of)
    weight = field_of(h_ref, 3)
    active = weight > 0.0
    places = [
        jnp.where(active, field_of(h_ref, axis) + base, 0.0)
        for axis, base in enumerate(cell_axes())
    ]
    speeds = [jnp.where(active, field_of(h_ref, 4 + axis), 0.0) for axis in range(3)]
    safe = jnp.where(active, rho_ref[...], 1.0)
    entropy = jnp.where(active, field_of(h_ref, 7), 1.0)
    root = jnp.exp(jnp.log(safe) * (1.0 / 3.0))
    sound = jnp.sqrt(GAMMA * entropy) * root
    press = entropy / root
    norm = split(places[0] * places[0] + places[1] * places[1] + places[2] * places[2])
    turn = split(4.0 * (places[0] * speeds[0] + places[1] * speeds[1] + places[2] * speeds[2]))
    one = jnp.ones_like(weight)
    zero = jnp.zeros_like(weight)
    square_rows, closing_rows, target_rows = [], [], []
    place_pieces = [split(place) for place in places]
    speed_pieces = [split(speed) for speed in speeds]
    for place, speed in zip(place_pieces, speed_pieces):
        for mine, theirs in PAIRS:
            target_rows.append(place[mine])
            square_rows.append(-2.0 * place[theirs])
            closing_rows.append(-4.0 * speed[theirs])
    for piece, other in zip(norm, turn):
        target_rows.append(one)
        square_rows.append(piece)
        closing_rows.append(other)
    for piece in norm:
        target_rows.append(piece)
        square_rows.append(one)
        closing_rows.append(zero)
    for place, speed in zip(place_pieces, speed_pieces):
        for mine, theirs in PAIRS:
            target_rows.append(speed[mine])
            square_rows.append(zero)
            closing_rows.append(-4.0 * place[theirs])
    for piece in turn:
        target_rows.append(piece)
        square_rows.append(zero)
        closing_rows.append(one)
    width = 48
    while len(target_rows) < width:
        target_rows.append(zero)
        square_rows.append(zero)
        closing_rows.append(zero)
    put_rows(source, square_rows, width)
    put_rows(extra, closing_rows, width)
    put_rows(target, target_rows, width)
    gather_rows = list(split(weight))
    for place in places:
        gather_rows.extend(split(weight * place))
    while len(gather_rows) < 16:
        gather_rows.append(zero)
    gather_rows[12] = sound
    gather_rows[13] = 4.0 * safe
    gather_rows[14] = press
    put_rows(gather, gather_rows, 16)

    keep = lax.broadcasted_iota(jnp.int32, (16, LANES), 0) < 12

    def convert(pair, carry):
        for half in range(2):
            tile = 2 * pair + half
            place = pl.ds(pl.multiple_of(tile * width, width), width)
            sums = gather[pl.ds(pl.multiple_of(tile * 16, 16), 16), :]
            masses = jnp.where(keep, sums, 0.0).astype(BF16)
            source16[tile, :, 0:LANES] = source[place, :].astype(BF16)
            source16[tile, :, LANES:] = extra[place, :].astype(BF16)
            gather16[tile, :, 0:LANES] = masses
            gather16[tile, :, LANES:] = masses
            fields[tile] = sums[8:16, :]
        return carry

    lax.fori_loop(0, CELLS, convert, 0)
    source16[EMPTY] = jnp.zeros((width, 2 * LANES), BF16)
    gather16[EMPTY] = jnp.zeros((16, 2 * LANES), BF16)
    fields[EMPTY] = jnp.ones((8, LANES), F32)
    for number, own in enumerate(own_cells()):
        for half in range(2):
            chunk = 2 * number + half
            tile = 2 * own + half
            target16[chunk] = target[tile * width : (tile + 1) * width, :].T.astype(BF16)
            for ref, row in ((mine_c, 12), (mine_r, 13), (mine_p, 14)):
                line = gather[tile * 16 + row : tile * 16 + row + 1, :]
                ref[chunk] = jnp.broadcast_to(line, (LANES, LANES)).T
    target16[2 * OWN] = jnp.zeros((LANES, width), BF16)
    for ref in (mine_c, mine_r, mine_p):
        ref[2 * OWN] = jnp.ones((LANES, LANES), F32)
    total_acc[...] = jnp.zeros_like(total_acc)
    force1[...] = jnp.zeros_like(force1)

    def distances(step, far):
        mine = target16[chunk_of[step]]
        start = first[step]
        for number in range(UNROLL):
            far[number] = jnp.dot(mine, source16[tiles[start + number]], preferred_element_type=F32)

    def forces(step, far, force):
        chunk = chunk_of[step]
        start = first[step]
        theirs = [fields[tiles[start + number]] for number in range(UNROLL)]
        for group in range(LANES // 16):
            for number in range(UNROLL):
                sound_j = theirs[number][4:5]
                rho_j = theirs[number][5:6]
                press_j = theirs[number][6:7]
                parts = []
                for sub in range(2):
                    rows = slice(group * 16 + sub * 8, group * 16 + sub * 8 + 8)
                    square = jnp.maximum(far[number, rows, 0:LANES], TINY)
                    closing = jnp.minimum(far[number, rows, LANES:], 0.0)
                    inverse = lax.rsqrt(square)
                    radius = square * inverse
                    clipped = jnp.maximum(1.0 - radius, 0.0)
                    slope = jnp.maximum(
                        2.0 - 3.0 * radius, jnp.minimum(clipped * clipped * inverse, 0.5)
                    )
                    soft = square + SOFTEN
                    both_rho = mine_r[chunk, rows, :] + rho_j
                    both_sound = mine_c[chunk, rows, :] + sound_j
                    both_press = mine_p[chunk, rows, :] + press_j
                    viscous = closing * (closing - both_sound * soft)
                    viscous = viscous / (soft * soft * both_rho)
                    parts.append((both_press + viscous) * slope)
                value = jnp.concatenate(parts, axis=0)
                high = value.astype(BF16)
                rows = slice(group * 16, group * 16 + 16)
                force[number, rows, 0:LANES] = high
                force[number, rows, LANES:] = (value - high.astype(F32)).astype(BF16)

    def collect(step, force):
        start = first[step]
        acc = None
        for number in range(UNROLL):
            part = lax.dot_general(
                force[number],
                gather16[tiles[start + number]],
                (((1,), (1,)), ((), ())),
                preferred_element_type=F32,
            )
            acc = part if acc is None else acc + part
        total_acc[chunk_of[step]] += acc

    distances(0, far0)

    def two_steps(pair, carry):
        step = 2 * pair
        distances(step + 1, far1)
        forces(step, far0, force0)
        collect(jnp.maximum(step - 1, 0), force1)
        distances(step + 2, far0)
        forces(step + 1, far1, force1)
        collect(step, force0)
        return carry

    pairs = (steps + 1) // 2
    lax.fori_loop(0, pairs, two_steps, 0)
    collect(2 * pairs - 1, force1)

    for number, own in enumerate(own_cells()):
        for half in range(2):
            sums = total_acc[2 * number + half].T
            part = slice(half * LANES, (half + 1) * LANES)
            mass = sums[0:1] + sums[1:2] + sums[2:3]
            top = (2 * own + half) * FIELDS
            shown = h_ref[top + 3 : top + 4, :] > 0.0
            for axis in range(3):
                moment = sums[3 + 3 * axis : 4 + 3 * axis] + sums[4 + 3 * axis : 5 + 3 * axis]
                moment = moment + sums[5 + 3 * axis : 6 + 3 * axis]
                offset = float((own // (WIDE * WIDE), own // WIDE % WIDE, own % WIDE)[axis] - 2)
                place = h_ref[top + axis : top + axis + 1, :] + offset
                value = (-6.0 * SIGMA) * (moment - place * mass)
                out_ref[axis, number : number + 1, part] = jnp.where(shown, value, 0.0)


def vmem():
    return pl.BlockSpec(memory_space=pltpu.VMEM)


def smem():
    return pl.BlockSpec(memory_space=pltpu.SMEM)


LISTS = [
    pltpu.SMEM((OWN * LIST + 64,), jnp.int32),
    pltpu.SMEM((MAX_STEPS + 8,), jnp.int32),
    pltpu.SMEM((MAX_STEPS + 8,), jnp.int32),
]


def density_call(full, near):
    return pl.pallas_call(
        density_kernel,
        out_shape=jax.ShapeDtypeStruct((OWN, SLOTS), F32),
        in_specs=[smem(), vmem()],
        out_specs=vmem(),
        scratch_shapes=[
            pltpu.VMEM((TILES * 32, LANES), F32),
            pltpu.VMEM((TILES * 32, LANES), F32),
            pltpu.VMEM((EMPTY + 1, 32, LANES), BF16),
            pltpu.VMEM((2 * OWN + 1, LANES, 32), BF16),
            pltpu.VMEM((EMPTY + 1, FIELDS, LANES), F32),
            pltpu.VMEM((UNROLL // 2, LANES, 2 * LANES), F32),
            pltpu.VMEM((UNROLL // 2, LANES, 2 * LANES), F32),
            pltpu.VMEM((2 * OWN + 1, LANES, LANES), F32),
        ]
        + LISTS,
        name="density",
    )(full, near)


def force_call(full, near, rho):
    return pl.pallas_call(
        force_kernel,
        out_shape=jax.ShapeDtypeStruct((3, OWN, SLOTS), F32),
        in_specs=[smem(), vmem(), vmem()],
        out_specs=vmem(),
        scratch_shapes=[
            pltpu.VMEM((TILES * 48, LANES), F32),
            pltpu.VMEM((TILES * 48, LANES), F32),
            pltpu.VMEM((TILES * 48, LANES), F32),
            pltpu.VMEM((TILES * 16, LANES), F32),
            pltpu.VMEM((EMPTY + 1, 48, 2 * LANES), BF16),
            pltpu.VMEM((2 * OWN + 1, LANES, 48), BF16),
            pltpu.VMEM((EMPTY + 1, 8, LANES), F32),
            pltpu.VMEM((EMPTY + 1, 16, 2 * LANES), BF16),
            pltpu.VMEM((2 * OWN + 1, LANES, LANES), F32),
            pltpu.VMEM((2 * OWN + 1, LANES, LANES), F32),
            pltpu.VMEM((2 * OWN + 1, LANES, LANES), F32),
            pltpu.VMEM((UNROLL, LANES, 2 * LANES), F32),
            pltpu.VMEM((UNROLL, LANES, 2 * LANES), F32),
            pltpu.VMEM((UNROLL, LANES, 2 * LANES), BF16),
            pltpu.VMEM((UNROLL, LANES, 2 * LANES), BF16),
            pltpu.VMEM((2 * OWN + 1, LANES, 16), F32),
        ]
        + LISTS,
        name="force",
    )(full, near, rho)


def exchange_kernel(own_ref, out_ref, local_sem, send_sem, recv_sem):
    sides = []
    for axis in ("gz", "gy", "gx"):
        count = lax.axis_size(axis)
        me = lax.axis_index(axis)
        sides.append((axis, lax.rem(me + 1, count), lax.rem(me + count - 1, count)))
    local = pltpu.make_async_copy(own_ref, out_ref.at[1:3, 1:3, 1:3], local_sem)
    local.start()
    barrier = pltpu.get_barrier_semaphore()
    for axis, up, down in sides:
        for other in (up, down):
            pl.semaphore_signal(
                barrier, inc=1, device_id={axis: other}, device_id_type=pl.DeviceIdType.MESH
            )
    pl.semaphore_wait(barrier, 6)
    for phase, (axis, up, down) in enumerate(sides):
        if axis == "gz":
            to_up, to_down = own_ref.at[:, :, 1:2], own_ref.at[:, :, 0:1]
            at_up, at_down = out_ref.at[1:3, 1:3, 0:1], out_ref.at[1:3, 1:3, 3:4]
        elif axis == "gy":
            to_up, to_down = out_ref.at[1:3, 2:3], out_ref.at[1:3, 1:2]
            at_up, at_down = out_ref.at[1:3, 0:1], out_ref.at[1:3, 3:4]
        else:
            to_up, to_down = out_ref.at[2:3], out_ref.at[1:2]
            at_up, at_down = out_ref.at[0:1], out_ref.at[3:4]
        copies = []
        for side, (source, dest, other) in enumerate(
            ((to_up, at_up, up), (to_down, at_down, down))
        ):
            copies.append(
                pltpu.make_async_remote_copy(
                    src_ref=source,
                    dst_ref=dest,
                    send_sem=send_sem.at[2 * phase + side],
                    recv_sem=recv_sem.at[2 * phase + side],
                    device_id={axis: other},
                    device_id_type=pl.DeviceIdType.MESH,
                )
            )
        for copy in copies:
            copy.start()
        if phase == 0:
            local.wait()
        for copy in copies:
            copy.wait()


def exchange_call(own, number):
    width, slots = own.shape[-2:]
    return pl.pallas_call(
        exchange_kernel,
        out_shape=jax.ShapeDtypeStruct((WIDE, WIDE, WIDE, width, slots), F32),
        in_specs=[vmem()],
        out_specs=vmem(),
        scratch_shapes=[
            pltpu.SemaphoreType.DMA,
            pltpu.SemaphoreType.DMA((6,)),
            pltpu.SemaphoreType.DMA((6,)),
        ],
        compiler_params=pltpu.CompilerParams(collective_id=number, has_side_effects=True),
        name=f"exchange{number}",
    )(own)


def per_device(positions, velocities, masses, entropy, counts):
    slot_ids = lax.broadcasted_iota(jnp.int32, masses.shape, 3)
    active = slot_ids < counts[..., None]
    weight = jnp.where(active, masses, 0.0)
    fields = [positions[0], positions[1], positions[2], weight]
    fields += [velocities[0], velocities[1], velocities[2], entropy]
    halves = masses.shape[:3] + (2, LANES)
    own = jnp.stack([field.reshape(halves) for field in fields], axis=4)
    near = exchange_call(own.reshape(masses.shape[:3] + (2 * FIELDS, LANES)), 0)
    full = (near[:, :, :, FIELDS + 3, 0].reshape(CELLS) > 0.0).astype(jnp.int32)
    near = near.reshape(TILES * FIELDS, LANES)
    raw = density_call(full, near).reshape(masses.shape)
    density = jnp.where(active, raw, 0.0)
    rho = exchange_call(density.reshape(halves), 1).reshape(TILES, LANES)
    accel = force_call(full, near, rho)
    return density, accel.reshape(positions.shape)


def solution(mesh):
    return jax.shard_map(
        per_device,
        mesh=mesh,
        in_specs=(
            P(None, "gx", "gy", "gz", None),
            P(None, "gx", "gy", "gz", None),
            P("gx", "gy", "gz", None),
            P("gx", "gy", "gz", None),
            P("gx", "gy", "gz"),
        ),
        out_specs=(P("gx", "gy", "gz", None), P(None, "gx", "gy", "gz", None)),
        check_vma=False,
    )
```

```python
import functools
import math

import jax
import jax.numpy as jnp
from jax import lax
from jax.experimental import pallas as pl
from jax.experimental.pallas import tpu as pltpu
from jax.sharding import PartitionSpec as P

SIGMA = 8.0 / math.pi
GAMMA = 5.0 / 3.0
SOFTEN = 0.01
TINY = 1e-12
SLOTS = 256
WIDE = 4
CELLS = WIDE * WIDE * WIDE
OWN = 8
LANES = 128
TILES = 2 * CELLS
EMPTY = TILES
UNROLL = 4
LIST = 64
ROWS = 4
GROUPS = 6
WIDTH = 8 * GROUPS
PADDED = EMPTY + 8
F32 = jnp.float32
BF16 = jnp.bfloat16


def cell_id(x, y, z):
    return (x * WIDE + y) * WIDE + z


def own_cells():
    return [cell_id(1 + n // 4, 1 + n // 2 % 2, 1 + n % 2) for n in range(OWN)]


def halo_neighbours(number):
    x, y, z = 1 + number // 4, 1 + number // 2 % 2, 1 + number % 2
    around = [
        cell_id(x + dx, y + dy, z + dz)
        for dx in (-1, 0, 1)
        for dy in (-1, 0, 1)
        for dz in (-1, 0, 1)
    ]
    return [other for other in around if other not in own_cells()]


def full_bits(near_ref):
    upper = near_ref[pl.ds(2 * ROWS - 1, CELLS, stride=2 * ROWS), :]
    power = jnp.ones((16, LANES), F32)
    ids = lax.broadcasted_iota(jnp.int32, (16, LANES), 0)
    for bit in range(4):
        power = jnp.where((ids & (1 << bit)) > 0, power * float(1 << (1 << bit)), power)
    first = lax.broadcasted_iota(jnp.int32, (16, LANES), 1) == 0
    bits = []
    for group in range(4):
        part = upper[16 * group : 16 * group + 16]
        bits.append(jnp.sum(jnp.where(first & (part > 0.0), power, 0.0)).astype(jnp.int32))
    return bits


def build_lists(full_of, tiles, order, count_of):
    total = jnp.int32(0)
    place = jnp.int32(0)
    for number, own in enumerate(own_cells()):
        where = jnp.int32(number * LIST)
        for other in halo_neighbours(number):
            tiles[where] = jnp.int32(2 * other)
            tiles[where + 1] = jnp.int32(2 * other + 1)
            where = where + 1 + full_of(other)
        for extra in range(UNROLL - 1):
            tiles[where + extra] = jnp.int32(EMPTY)
        count = (where - number * LIST + UNROLL - 1) // UNROLL
        for half in range(2):
            order[place] = jnp.int32(2 * number + half)
            count_of[place] = count
            used = 1 if half == 0 else full_of(own)
            place = place + used
            total = total + used * count
    order[place] = jnp.int32(2 * OWN)
    count_of[place] = jnp.int32(1 << 20)
    for extra in range(4 * UNROLL):
        tiles[OWN * LIST + extra] = jnp.int32(EMPTY)
    return total


def listed(tiles, order, count_of):
    def advance(state):
        place, step = state
        more = step + 1 < count_of[place]
        return jnp.where(more, place, place + 1), jnp.where(more, step + 1, 0)

    def where_is(state):
        chunk = order[state[0]]
        start = (chunk >> 1) * LIST + state[1] * UNROLL
        return chunk, [tiles[start + number] for number in range(UNROLL)]

    return advance, where_is


def own_walk():
    def advance(state):
        return (jnp.minimum(state[0] + 1, OWN * OWN - 1),)

    def where_is(state):
        first = (state[0] & 3) * UNROLL
        return state[0] >> 2, [first + number for number in range(UNROLL)]

    return advance, where_is


def split(value):
    high = value.astype(BF16).astype(F32)
    rest = value - high
    middle = rest.astype(BF16).astype(F32)
    low = rest - middle
    return high, middle, low


PAIRS = ((0, 0), (0, 1), (1, 0), (1, 1), (0, 2), (2, 0))


def tile_rows(place, half, speed=None):
    if half:
        place = pltpu.roll(place, 4, 0)
    elif speed is not None:
        speed = pltpu.roll(speed, 4, 0)
    row = lax.broadcasted_iota(jnp.int32, (8, LANES), 0)
    return jnp.where(row < 4, place, 0.0 if speed is None else speed)


def cell_base(cell):
    row = lax.broadcasted_iota(jnp.int32, (8, LANES), 0)
    x, y, z = [
        (value - 2).astype(F32) for value in (cell >> 4, (cell >> 2) & 3, cell & 3)
    ]
    return jnp.where(row == 0, x, jnp.where(row == 1, y, jnp.where(row == 2, z, 0.0)))


def stack_groups(groups):
    return jnp.concatenate(groups, axis=0)


class Tile:
    def __init__(self, rows, base, moving):
        row = lax.broadcasted_iota(jnp.int32, (8, LANES), 0)
        self.moving = moving
        self.row = row
        self.is_x = row < 3
        self.is_xv = (row < 3) | ((row >= 4) & (row < 7))
        self.weight = jnp.broadcast_to(rows[3:4], (8, LANES))
        self.values = jnp.where((self.weight > 0.0) & self.is_xv, rows + base, 0.0)
        self.pieces = split(self.values)
        squares = self.values * self.values
        self.norm = split(self.fold(squares))
        if moving:
            self.turn = split(4.0 * self.fold(self.values * pltpu.roll(self.values, 4, 0)))

    def fold(self, value):
        total = jnp.sum(jnp.where(self.is_x, value, 0.0), axis=0, keepdims=True)
        return jnp.broadcast_to(total, (8, LANES))

    def place(self, value, third, seventh):
        rest = jnp.where(self.row == 3, third, jnp.where(self.row == 7, seventh, 0.0))
        return jnp.where(self.is_xv, value, rest)

    def target(self):
        groups = []
        for group, (mine, _) in enumerate(PAIRS):
            if group < 3:
                groups.append(self.place(self.pieces[mine], 1.0, self.norm[group]))
            else:
                third = self.turn[group - 3] if self.moving else 0.0
                groups.append(self.place(self.pieces[mine], third, 0.0))
        return stack_groups(groups)

    def square(self):
        groups = []
        scaled = [jnp.where(self.is_x, -2.0 * piece, 0.0) for piece in self.pieces]
        for group, (_, theirs) in enumerate(PAIRS):
            if group < 3:
                groups.append(self.place(scaled[theirs], self.norm[group], 1.0))
            else:
                groups.append(scaled[theirs])
        return stack_groups(groups).astype(BF16)

    def closing(self):
        groups = []
        scaled = [-4.0 * pltpu.roll(piece, 4, 0) for piece in self.pieces]
        for group, (_, theirs) in enumerate(PAIRS):
            third = self.turn[group] if group < 3 else 1.0
            groups.append(self.place(scaled[theirs], third, 0.0))
        return stack_groups(groups).astype(BF16)

    def gather(self):
        moments = jnp.where(self.is_x, self.values * self.weight, 0.0)
        moments = jnp.where(self.row == 3, self.weight, moments)
        high, middle, low = split(moments)
        first = jnp.where(self.row < 4, high, pltpu.roll(middle, 4, 0))
        return stack_groups([first, jnp.where(self.row < 4, low, 0.0)]).astype(BF16)


def pipelined(walk, first, pairs, distances, work, collect, far, kept, previous):
    advance, where_is = walk

    def turn(_, carry):
        last, now = carry
        later = advance(now)
        after = advance(later)
        distances(where_is(later), far[1])
        work(where_is(now), far[0], kept[0])
        collect(where_is(last), kept[1])
        distances(where_is(after), far[0])
        work(where_is(later), far[1], kept[1])
        collect(where_is(now), kept[0])
        return later, after

    return lax.fori_loop(0, pairs, turn, (previous, first))


def density_parts(target16, source16, weights, total_acc):
    def distances(step, far):
        chunk, ids = step
        mine = target16[chunk]
        for pair in range(UNROLL // 2):
            both = jnp.concatenate([source16[ids[2 * pair]], source16[ids[2 * pair + 1]]], axis=1)
            far[pair] = jnp.dot(mine, both, preferred_element_type=F32)

    def add(step, far, _):
        chunk, ids = step
        mass = [weights[pl.ds(tile, 1), :] for tile in ids]
        for group in range(LANES // 8):
            rows = slice(group * 8, group * 8 + 8)
            acc = total_acc[chunk, rows, :]
            for number in range(UNROLL):
                lanes = slice((number % 2) * LANES, (number % 2 + 1) * LANES)
                square = jnp.maximum(far[number // 2, rows, lanes], TINY)
                radius = square * lax.rsqrt(square)
                rest = 1.0 - radius
                near = 0.5 - 3.0 * (square * rest)
                clipped = jnp.maximum(rest, 0.0)
                value = jnp.minimum(near, clipped * clipped * clipped)
                acc = acc + value * mass[number]
            total_acc[chunk, rows, :] = acc

    def collect(step, kept):
        pass

    return distances, add, collect


def density_rows(total_acc, chunk):
    return (2.0 * SIGMA) * jnp.sum(total_acc[chunk].T, axis=0, keepdims=True)


def force_parts(target16, source16, gather16, sound, rho, press, mine, total_acc):
    mine_c, mine_r, mine_p = mine

    def distances(step, far):
        chunk, ids = step
        for number, tile in enumerate(ids):
            far[number] = jnp.dot(target16[chunk], source16[tile], preferred_element_type=F32)

    def forces(step, far, force):
        chunk, ids = step
        sound_j = [sound[pl.ds(tile, 1), :] for tile in ids]
        rho_j = [rho[pl.ds(tile, 1), :] for tile in ids]
        press_j = [press[pl.ds(tile, 1), :] for tile in ids]
        for group in range(LANES // 16):
            for number in range(UNROLL):
                parts = []
                for sub in range(2):
                    rows = slice(group * 16 + sub * 8, group * 16 + sub * 8 + 8)
                    square = jnp.maximum(far[number, rows, 0:LANES], TINY)
                    closing = jnp.minimum(far[number, rows, LANES:], 0.0)
                    inverse = lax.rsqrt(square)
                    radius = square * inverse
                    clipped = jnp.maximum(1.0 - radius, 0.0)
                    slope = jnp.maximum(
                        2.0 - 3.0 * radius, jnp.minimum(clipped * clipped * inverse, 0.5)
                    )
                    soft = square + SOFTEN
                    both_rho = mine_r[chunk, rows, :] + rho_j[number]
                    both_sound = mine_c[chunk, rows, :] + sound_j[number]
                    both_press = mine_p[chunk, rows, :] + press_j[number]
                    viscous = closing * (closing - both_sound * soft)
                    viscous = viscous / (soft * soft * both_rho)
                    parts.append((both_press + viscous) * slope)
                value = jnp.concatenate(parts, axis=0)
                high = value.astype(BF16)
                rows = slice(group * 16, group * 16 + 16)
                force[number, rows, 0:LANES] = high
                force[number, rows, LANES:] = (value - high.astype(F32)).astype(BF16)

    def collect(step, force):
        chunk, ids = step
        acc = None
        for number, tile in enumerate(ids):
            part = lax.dot_general(
                force[number],
                gather16[tile],
                (((1,), (1,)), ((), ())),
                preferred_element_type=F32,
            )
            acc = part if acc is None else acc + part
        total_acc[chunk] += acc

    return distances, forces, collect


def states_of(weight, density, entropy):
    active = weight > 0.0
    safe = jnp.where(active, density, 1.0)
    entropy = jnp.where(active, entropy, 1.0)
    root = jnp.exp(jnp.log(safe) * (1.0 / 3.0))
    return jnp.sqrt(GAMMA * entropy) * root, 4.0 * safe, entropy / root


def spread(ref, chunk, line):
    ref[chunk] = jnp.broadcast_to(line, (LANES, LANES)).T


class Exchange:
    def __init__(self, arrays, local_sem, send_sem, recv_sem):
        self.arrays = arrays
        self.send_sem, self.recv_sem = send_sem, recv_sem
        self.local = [
            pltpu.make_async_copy(own, near.at[1:3, 1:3, 1:3], local_sem.at[number])
            for number, (own, near) in enumerate(arrays)
        ]
        self.moved = {
            axis: {
                0: lax.axis_index(axis),
                1: lax.rem(lax.axis_index(axis) + 1, lax.axis_size(axis)),
                -1: lax.rem(lax.axis_index(axis) + lax.axis_size(axis) - 1, lax.axis_size(axis)),
            }
            for axis in ("gx", "gy", "gz")
        }
        self.plane = [(dy, dz) for dz in (-1, 1) for dy in (-1, 0, 1)] + [(-1, 0), (1, 0)]
        self.count = 0

    def device(self, dx, dy, dz):
        return {
            "gx": self.moved["gx"][dx],
            "gy": self.moved["gy"][dy],
            "gz": self.moved["gz"][dz],
        }

    def greet(self):
        barrier = pltpu.get_barrier_semaphore()
        others = [(0, dy, dz) for dy, dz in self.plane] + [(-1, 0, 0), (1, 0, 0)]
        for other in others:
            pl.semaphore_signal(
                barrier,
                inc=1,
                device_id=self.device(*other),
                device_id_type=pl.DeviceIdType.MESH,
            )
        for copy in self.local:
            copy.start()

    def send(self, source, dest, other):
        copy = pltpu.make_async_remote_copy(
            src_ref=source,
            dst_ref=dest,
            send_sem=self.send_sem.at[self.count],
            recv_sem=self.recv_sem.at[self.count],
            device_id=self.device(*other),
            device_id_type=pl.DeviceIdType.MESH,
        )
        self.count += 1
        copy.start()
        return copy

    def start_plane(self):
        pl.semaphore_wait(pltpu.get_barrier_semaphore(), len(self.plane) + 2)
        taken = {-1: slice(0, 1), 0: slice(0, 2), 1: slice(1, 2)}
        landed = {-1: slice(3, 4), 0: slice(1, 3), 1: slice(0, 1)}
        self.copies = [
            self.send(
                own.at[:, taken[dy], taken[dz]], near.at[1:3, landed[dy], landed[dz]], (0, dy, dz)
            )
            for own, near in self.arrays
            for dy, dz in self.plane
        ]

    def start_gx(self):
        for copy in self.local + self.copies:
            copy.wait()
        self.copies = []
        for _, near in self.arrays:
            self.copies.append(self.send(near.at[2:3], near.at[0:1], (1, 0, 0)))
            self.copies.append(self.send(near.at[1:2], near.at[3:4], (-1, 0, 0)))

    def finish(self):
        for copy in self.copies:
            copy.wait()


def exchange_sems(arrays):
    return [
        pltpu.SemaphoreType.DMA((arrays,)),
        pltpu.SemaphoreType.DMA((10 * arrays,)),
        pltpu.SemaphoreType.DMA((10 * arrays,)),
    ]


def staged(walk, parts, distances, work, collect, far, kept, exchange):
    advance, where_is = walk
    state = (jnp.int32(0),)
    distances(where_is(state), far[0])
    carry = (state, state)
    for number, pairs in enumerate(parts):
        carry = pipelined(
            walk, carry[1], pairs, distances, work, collect, far, kept, carry[0]
        )
        (exchange.start_plane, exchange.start_gx, exchange.finish)[number]()
    return carry[0]


DENSITY_PARTS = (10, 21, 1)
FORCE_PARTS = (6, 20, 6)


def own_cell_rows(ref, number):
    return ref[number // 4, number // 2 % 2, number % 2]


def first_kernel(own_ref, near_ref, partial_ref, target16, source16, weights, far0, far1, total_acc, local_sem, send_sem, recv_sem):
    exchange = Exchange([(own_ref, near_ref)], local_sem, send_sem, recv_sem)
    exchange.greet()
    for number, own in enumerate(own_cells()):
        base = cell_base(jnp.int32(own))
        rows = own_cell_rows(own_ref, number)
        for half in range(2):
            chunk = 2 * number + half
            tile = Tile(tile_rows(rows, half), base, False)
            target16[chunk] = tile.target().T.astype(BF16)
            source16[chunk] = tile.square()
            weights[chunk : chunk + 1, :] = tile.weight[0:1]
    target16[2 * OWN] = jnp.zeros((LANES, WIDTH), BF16)
    total_acc[...] = jnp.zeros_like(total_acc)
    parts = density_parts(target16, source16, weights, total_acc)
    staged(own_walk(), DENSITY_PARTS, *parts, (far0, far1), (None, None), exchange)
    for chunk in range(2 * OWN):
        partial_ref[chunk : chunk + 1, :] = density_rows(total_acc, chunk)


def density_kernel(near_ref, partial_ref, target16, out_ref, own_ref, source16, weights, far0, far1, total_acc, tiles, order, count_of):
    bits = full_bits(near_ref)

    def full_of(cell):
        return (bits[cell // 16] >> (cell % 16)) & 1

    steps = build_lists(full_of, tiles, order, count_of)
    weights[0:EMPTY, :] = near_ref[pl.ds(3, TILES, stride=ROWS), :]
    weights[EMPTY:PADDED, :] = jnp.zeros((8, LANES), F32)

    def prepare(cell, carry):
        base = cell_base(cell)
        rows = near_ref[pl.ds(pl.multiple_of(cell * 8, 8), 8), :]
        for half in range(2):
            tile = Tile(tile_rows(rows, half), base, False)
            source16[2 * cell + half] = tile.square()
        return carry

    lax.fori_loop(0, CELLS, prepare, 0)
    source16[EMPTY] = jnp.zeros((WIDTH, LANES), BF16)
    total_acc[...] = jnp.zeros_like(total_acc)
    walk = listed(tiles, order, count_of)
    distances, add, collect = density_parts(target16, source16, weights, total_acc)
    first = (jnp.int32(0), jnp.int32(0))
    distances(walk[1](first), far0)
    pipelined(
        walk, first, (steps + 1) // 2, distances, add, collect, (far0, far1), (None, None), first
    )
    for number, own in enumerate(own_cells()):
        x, y, z = number // 4, number // 2 % 2, number % 2
        for half in range(2):
            chunk = 2 * number + half
            part = slice(half * LANES, (half + 1) * LANES)
            row = (2 * own + half) * ROWS + 3
            value = partial_ref[chunk : chunk + 1, :] + density_rows(total_acc, chunk)
            value = jnp.where(near_ref[row : row + 1, :] > 0.0, value, 0.0)
            out_ref[x, y, z : z + 1, part] = value
            own_ref[x, y, z, half : half + 1, :] = value


def second_kernel(place_ref, speed_ref, rho_ref, near_speed_ref, near_rho_ref, partial_ref, target16, source16, gather16, sound, rho, press, mine_c, mine_r, mine_p, far0, far1, force0, force1, total_acc, local_sem, send_sem, recv_sem):
    exchange = Exchange(
        [(speed_ref, near_speed_ref), (rho_ref, near_rho_ref)], local_sem, send_sem, recv_sem
    )
    exchange.greet()
    for number, own in enumerate(own_cells()):
        base = cell_base(jnp.int32(own))
        places = own_cell_rows(place_ref, number)
        speeds = own_cell_rows(speed_ref, number)
        density = own_cell_rows(rho_ref, number)
        for half in range(2):
            chunk = 2 * number + half
            rows = tile_rows(places, half, speeds)
            tile = Tile(rows, base, True)
            target16[chunk] = tile.target().T.astype(BF16)
            source16[chunk, :, 0:LANES] = tile.square()
            source16[chunk, :, LANES:] = tile.closing()
            masses = tile.gather()
            gather16[chunk, :, 0:LANES] = masses
            gather16[chunk, :, LANES:] = masses
            states = states_of(rows[3:4], density[half : half + 1], rows[7:8])
            for value, far, mine in zip(states, (sound, rho, press), (mine_c, mine_r, mine_p)):
                far[chunk : chunk + 1, :] = value
                spread(mine, chunk, value)
    target16[2 * OWN] = jnp.zeros((LANES, WIDTH), BF16)
    total_acc[...] = jnp.zeros_like(total_acc)
    force1[...] = jnp.zeros_like(force1)
    parts = force_parts(
        target16, source16, gather16, sound, rho, press, (mine_c, mine_r, mine_p), total_acc
    )
    walk = own_walk()
    last = staged(walk, FORCE_PARTS, *parts, (far0, far1), (force0, force1), exchange)
    parts[2](walk[1](last), force1)
    for chunk in range(2 * OWN):
        partial_ref[chunk] = total_acc[chunk].T


def force_kernel(near_ref, speed_ref, rho_ref, partial_ref, target16, out_ref, source16, gather16, sound, rho, press, mine_c, mine_r, mine_p, far0, far1, force0, force1, total_acc, tiles, order, count_of):
    bits = full_bits(near_ref)

    def full_of(cell):
        return (bits[cell // 16] >> (cell % 16)) & 1

    steps = build_lists(full_of, tiles, order, count_of)
    states = states_of(
        near_ref[pl.ds(3, TILES, stride=ROWS), :],
        rho_ref[...],
        speed_ref[pl.ds(3, TILES, stride=ROWS), :],
    )
    for value, ref in zip(states, (sound, rho, press)):
        ref[0:EMPTY, :] = value
        ref[EMPTY:PADDED, :] = jnp.ones((8, LANES), F32)

    def prepare(cell, carry):
        base = cell_base(cell)
        place = pl.ds(pl.multiple_of(cell * 8, 8), 8)
        for half in range(2):
            tile = Tile(tile_rows(near_ref[place, :], half, speed_ref[place, :]), base, True)
            number = 2 * cell + half
            source16[number, :, 0:LANES] = tile.square()
            source16[number, :, LANES:] = tile.closing()
            masses = tile.gather()
            gather16[number, :, 0:LANES] = masses
            gather16[number, :, LANES:] = masses
        return carry

    lax.fori_loop(0, CELLS, prepare, 0)
    source16[EMPTY] = jnp.zeros((WIDTH, 2 * LANES), BF16)
    gather16[EMPTY] = jnp.zeros((16, 2 * LANES), BF16)
    for number, own in enumerate(own_cells()):
        for half in range(2):
            line = slice(2 * own + half, 2 * own + half + 1)
            for ref, mine in ((sound, mine_c), (rho, mine_r), (press, mine_p)):
                spread(mine, 2 * number + half, ref[line, :])
    for mine in (mine_c, mine_r, mine_p):
        mine[2 * OWN] = jnp.ones((LANES, LANES), F32)
    total_acc[...] = jnp.zeros_like(total_acc)
    force1[...] = jnp.zeros_like(force1)
    walk = listed(tiles, order, count_of)
    distances, forces, collect = force_parts(
        target16, source16, gather16, sound, rho, press, (mine_c, mine_r, mine_p), total_acc
    )
    first = (jnp.int32(0), jnp.int32(0))
    distances(walk[1](first), far0)
    last, _ = pipelined(
        walk, first, (steps + 1) // 2, distances, forces, collect, (far0, far1), (force0, force1), first
    )
    collect(walk[1](last), force1)
    for number, own in enumerate(own_cells()):
        x, y, z = number // 4, number // 2 % 2, number % 2
        for half in range(2):
            chunk = 2 * number + half
            sums = total_acc[chunk].T + partial_ref[chunk]
            sums = sums[0:4] + sums[4:8] + sums[8:12]
            top = (2 * own + half) * ROWS
            shown = near_ref[top + 3 : top + 4, :] > 0.0
            part = slice(half * LANES, (half + 1) * LANES)
            for axis in range(3):
                offset = float((own // 16, own // 4 % 4, own % 4)[axis] - 2)
                place = near_ref[top + axis : top + axis + 1, :] + offset
                value = (-6.0 * SIGMA) * (sums[axis : axis + 1] - place * sums[3:4])
                out_ref[axis, x, y, z : z + 1, part] = jnp.where(shown, value, 0.0)


def vmem(number):
    return [pl.BlockSpec(memory_space=pltpu.VMEM) for _ in range(number)]


LISTS = [
    pltpu.SMEM((OWN * LIST + LIST,), jnp.int32),
    pltpu.SMEM((2 * OWN + 8,), jnp.int32),
    pltpu.SMEM((2 * OWN + 8,), jnp.int32),
]
CELL_BLOCK = (2 * ROWS, LANES)
NEAR = (WIDE, WIDE, WIDE)
TARGETS = jax.ShapeDtypeStruct((2 * OWN + 1, LANES, WIDTH), BF16)


def first_call(own):
    return pl.pallas_call(
        first_kernel,
        out_shape=(
            jax.ShapeDtypeStruct(NEAR + CELL_BLOCK, F32),
            jax.ShapeDtypeStruct((2 * OWN, LANES), F32),
            TARGETS,
        ),
        in_specs=vmem(1),
        out_specs=tuple(vmem(3)),
        scratch_shapes=[
            pltpu.VMEM((2 * OWN, WIDTH, LANES), BF16),
            pltpu.VMEM((2 * OWN, LANES), F32),
            pltpu.VMEM((UNROLL // 2, LANES, 2 * LANES), F32),
            pltpu.VMEM((UNROLL // 2, LANES, 2 * LANES), F32),
            pltpu.VMEM((2 * OWN + 1, LANES, LANES), F32),
        ]
        + exchange_sems(1),
        compiler_params=pltpu.CompilerParams(collective_id=0, has_side_effects=True),
        name="first",
    )(own)


def density_call(near, partial, targets):
    return pl.pallas_call(
        density_kernel,
        out_shape=(
            jax.ShapeDtypeStruct((2, 2, 2, SLOTS), F32),
            jax.ShapeDtypeStruct((2, 2, 2, 2, LANES), F32),
        ),
        in_specs=vmem(3),
        out_specs=tuple(vmem(2)),
        scratch_shapes=[
            pltpu.VMEM((EMPTY + 1, WIDTH, LANES), BF16),
            pltpu.VMEM((PADDED, LANES), F32),
            pltpu.VMEM((UNROLL // 2, LANES, 2 * LANES), F32),
            pltpu.VMEM((UNROLL // 2, LANES, 2 * LANES), F32),
            pltpu.VMEM((2 * OWN + 1, LANES, LANES), F32),
        ]
        + LISTS,
        name="density",
    )(near, partial, targets)


def force_scratch(tiles, padded):
    block = pltpu.VMEM((2 * OWN + 1, LANES, LANES), F32)
    return [
        pltpu.VMEM((tiles, WIDTH, 2 * LANES), BF16),
        pltpu.VMEM((tiles, 16, 2 * LANES), BF16),
        pltpu.VMEM((padded, LANES), F32),
        pltpu.VMEM((padded, LANES), F32),
        pltpu.VMEM((padded, LANES), F32),
        block,
        block,
        block,
        pltpu.VMEM((UNROLL, LANES, 2 * LANES), F32),
        pltpu.VMEM((UNROLL, LANES, 2 * LANES), F32),
        pltpu.VMEM((UNROLL, LANES, 2 * LANES), BF16),
        pltpu.VMEM((UNROLL, LANES, 2 * LANES), BF16),
        pltpu.VMEM((2 * OWN + 1, LANES, 16), F32),
    ]


def second_call(place, speed, rho):
    return pl.pallas_call(
        second_kernel,
        out_shape=(
            jax.ShapeDtypeStruct(NEAR + CELL_BLOCK, F32),
            jax.ShapeDtypeStruct(NEAR + (2, LANES), F32),
            jax.ShapeDtypeStruct((2 * OWN, 16, LANES), F32),
            TARGETS,
        ),
        in_specs=vmem(3),
        out_specs=tuple(vmem(4)),
        scratch_shapes=force_scratch(2 * OWN, 2 * OWN) + exchange_sems(2),
        compiler_params=pltpu.CompilerParams(collective_id=1, has_side_effects=True),
        name="second",
    )(place, speed, rho)


def force_call(near, speed, rho, partial, targets):
    return pl.pallas_call(
        force_kernel,
        out_shape=jax.ShapeDtypeStruct((3, 2, 2, 2, SLOTS), F32),
        in_specs=vmem(5),
        out_specs=vmem(1)[0],
        scratch_shapes=force_scratch(EMPTY + 1, PADDED) + LISTS,
        name="force",
    )(near, speed, rho, partial, targets)


def per_device(positions, velocities, masses, entropy, counts):
    slot_ids = lax.broadcasted_iota(jnp.int32, masses.shape, 3)
    weight = jnp.where(slot_ids < counts[..., None], masses, 0.0)
    halves = masses.shape[:3] + (2, LANES)

    def blocks(parts):
        joined = jnp.stack([part.reshape(halves) for part in parts], axis=4)
        return joined.reshape(masses.shape[:3] + CELL_BLOCK)

    place = blocks([positions[0], positions[1], positions[2], weight])
    speed = blocks([velocities[0], velocities[1], velocities[2], entropy])
    near, partial, targets = first_call(place)
    near = near.reshape(CELLS * 8, LANES)
    density, own_rho = density_call(near, partial, targets)
    near_speed, near_rho, sums, targets = second_call(place, speed, own_rho)
    accel = force_call(
        near, near_speed.reshape(CELLS * 8, LANES), near_rho.reshape(TILES, LANES), sums, targets
    )
    return density, accel


def solution(mesh):
    return jax.shard_map(
        per_device,
        mesh=mesh,
        in_specs=(
            P(None, "gx", "gy", "gz", None),
            P(None, "gx", "gy", "gz", None),
            P("gx", "gy", "gz", None),
            P("gx", "gy", "gz", None),
            P("gx", "gy", "gz"),
        ),
        out_specs=(P("gx", "gy", "gz", None), P(None, "gx", "gy", "gz", None)),
        check_vma=False,
    )
```

```python
import functools
import math

import jax
import jax.numpy as jnp
from jax import lax
from jax.experimental import pallas as pl
from jax.experimental.pallas import tpu as pltpu
from jax.sharding import PartitionSpec as P

SIGMA = 8.0 / math.pi
GAMMA = 5.0 / 3.0
SOFTEN = 0.01
TINY = 1e-12
SLOTS = 256
WIDE = 4
CELLS = WIDE * WIDE * WIDE
OWN = 8
LANES = 128
TILES = 2 * CELLS
UNITS = 2 * TILES
UNROLL = 4
LIST = 128
ORDER_AT = 9 * LIST
COUNT_AT = ORDER_AT + 24
NEEDED_AT = COUNT_AT + 24
TOTAL_AT = NEEDED_AT + 144
PLAN = 11 * LIST
PREPARED = 4
HALF = LANES // 2
ROWS = 4
GROUPS = 6
WIDTH = 8 * GROUPS
PADDED = UNITS + 8
F32 = jnp.float32
BF16 = jnp.bfloat16


def cell_id(x, y, z):
    return (x * WIDE + y) * WIDE + z


def own_cells():
    return [cell_id(1 + n // 4, 1 + n // 2 % 2, 1 + n % 2) for n in range(OWN)]


def halo_neighbours(number):
    x, y, z = 1 + number // 4, 1 + number // 2 % 2, 1 + number % 2
    around = [
        cell_id(x + dx, y + dy, z + dz)
        for dx in (-1, 0, 1)
        for dy in (-1, 0, 1)
        for dz in (-1, 0, 1)
    ]
    return [other for other in around if other not in own_cells()]


def unit_bits(near_ref):
    lower = near_ref[pl.ds(ROWS - 1, CELLS, stride=2 * ROWS), :]
    upper = near_ref[pl.ds(2 * ROWS - 1, CELLS, stride=2 * ROWS), :]
    ids = lax.broadcasted_iota(jnp.int32, (8, LANES), 0)
    lanes = lax.broadcasted_iota(jnp.int32, (8, LANES), 1)
    power = jnp.ones((8, LANES), F32)
    for bit in range(3):
        power = jnp.where((ids & (1 << bit)) > 0, power * float(4 ** (1 << bit)), power)
    bits = []
    for group in range(CELLS // 8):
        part = slice(8 * group, 8 * group + 8)
        middle = lanes == HALF
        value = jnp.where(middle & (lower[part] > 0.0), power, 0.0)
        value = value + jnp.where((middle | (lanes == 0)) & (upper[part] > 0.0), power, 0.0)
        bits.append(jnp.sum(value).astype(jnp.int32))

    def extra_of(cell):
        return (bits[cell // 8] >> (2 * (cell % 8))) & 3

    return extra_of


class View:
    def __init__(self, plan, base):
        self.plan, self.base = plan, base

    def __getitem__(self, index):
        return self.plan[self.base + index]

    def __setitem__(self, index, value):
        self.plan[self.base + index] = value


def views(plan):
    return [View(plan, base) for base in (0, ORDER_AT, COUNT_AT, NEEDED_AT, TOTAL_AT)]


def build_plan(extra_of, plan):
    tiles, order, count_of, needed, totals = views(plan)
    used = jnp.int32(0)
    for cell in range(CELLS):
        if cell in own_cells():
            continue
        needed[used] = jnp.int32(2 * cell)
        needed[used + 1] = jnp.int32(2 * cell + 1)
        used = used + 1 + (extra_of(cell) >> 1)
    for extra in range(PREPARED - 1):
        needed[used + extra] = jnp.int32(0)
    totals[1] = used
    total = jnp.int32(0)
    place = jnp.int32(0)
    for number, own in enumerate(own_cells()):
        where = jnp.int32(number * LIST)
        for other in halo_neighbours(number):
            for unit in range(4):
                tiles[where + unit] = jnp.int32(4 * other + unit)
            where = where + 1 + extra_of(other)
        for extra in range(2 * UNROLL - 1):
            tiles[where + extra] = jnp.int32(UNITS)
        count = (where - number * LIST + 2 * UNROLL - 1) // (2 * UNROLL)
        for half in range(2):
            order[place] = jnp.int32(2 * number + half)
            count_of[place] = count
            used = 1 if half == 0 else extra_of(own) >> 1
            place = place + used
            total = total + used * count
    order[place] = jnp.int32(2 * OWN)
    count_of[place] = jnp.int32(1 << 20)
    for extra in range(12 * UNROLL):
        tiles[OWN * LIST + extra] = jnp.int32(UNITS)
    totals[0] = total


def listed(plan):
    tiles, order, count_of, _, _ = views(plan)

    def advance(state):
        place, step = state
        more = step + 1 < count_of[place]
        return jnp.where(more, place, place + 1), jnp.where(more, step + 1, 0)

    def where_is(state):
        chunk = order[state[0]]
        start = (chunk >> 1) * LIST + state[1] * (2 * UNROLL)
        units = [tiles[start + number] for number in range(2 * UNROLL)]
        return chunk, [(units[2 * n], units[2 * n + 1] ^ 1) for n in range(UNROLL)]

    return advance, where_is


def pick(ref, tile):
    if not isinstance(tile, tuple):
        return ref[tile]
    low, high = tile
    lanes = lax.broadcasted_iota(jnp.int32, ref.shape[1:], 1)
    return jnp.where((lanes & HALF) == 0, ref[low], ref[high])


def pick_row(ref, tile):
    if not isinstance(tile, tuple):
        return ref[pl.ds(tile, 1), :]
    low, high = tile
    lanes = lax.broadcasted_iota(jnp.int32, (1, LANES), 1)
    return jnp.where((lanes & HALF) == 0, ref[pl.ds(low, 1), :], ref[pl.ds(high, 1), :])


def turned(value):
    return pltpu.roll(value, HALF, 1)


def put_both(ref, value):
    ref[pl.ds(0, TILES, stride=2), :] = value
    ref[pl.ds(1, TILES, stride=2), :] = turned(value)


def own_walk():
    def advance(state):
        return (jnp.minimum(state[0] + 1, OWN * OWN - 1),)

    def where_is(state):
        first = (state[0] & 3) * UNROLL
        return state[0] >> 2, [first + number for number in range(UNROLL)]

    return advance, where_is


def split(value):
    high = value.astype(BF16).astype(F32)
    rest = value - high
    middle = rest.astype(BF16).astype(F32)
    low = rest - middle
    return high, middle, low


PAIRS = ((0, 0), (0, 1), (1, 0), (1, 1), (0, 2), (2, 0))


def needed_tiles(plan, turn):
    needed = views(plan)[3]
    return [needed[turn * PREPARED + number] for number in range(PREPARED)]


def choose_rows(place, half, speed=None):
    other = pltpu.roll(place, 4, 0)
    row = lax.broadcasted_iota(jnp.int32, (8, LANES), 0)
    place = jnp.where(half > 0, other, place)
    if speed is None:
        return jnp.where(row < 4, place, 0.0)
    return jnp.where(row < 4, place, jnp.where(half > 0, speed, pltpu.roll(speed, 4, 0)))


def tile_rows(place, half, speed=None):
    if half:
        place = pltpu.roll(place, 4, 0)
    elif speed is not None:
        speed = pltpu.roll(speed, 4, 0)
    row = lax.broadcasted_iota(jnp.int32, (8, LANES), 0)
    return jnp.where(row < 4, place, 0.0 if speed is None else speed)


def cell_base(cell):
    row = lax.broadcasted_iota(jnp.int32, (8, LANES), 0)
    x, y, z = [
        (value - 2).astype(F32) for value in (cell >> 4, (cell >> 2) & 3, cell & 3)
    ]
    return jnp.where(row == 0, x, jnp.where(row == 1, y, jnp.where(row == 2, z, 0.0)))


def stack_groups(groups):
    return jnp.concatenate(groups, axis=0)


class Tile:
    def __init__(self, rows, base, moving):
        row = lax.broadcasted_iota(jnp.int32, (8, LANES), 0)
        self.moving = moving
        self.row = row
        self.is_x = row < 3
        self.is_xv = (row < 3) | ((row >= 4) & (row < 7))
        self.weight = jnp.broadcast_to(rows[3:4], (8, LANES))
        self.values = jnp.where((self.weight > 0.0) & self.is_xv, rows + base, 0.0)
        self.pieces = split(self.values)
        squares = self.values * self.values
        self.norm = split(self.fold(squares))
        if moving:
            self.turn = split(4.0 * self.fold(self.values * pltpu.roll(self.values, 4, 0)))

    def fold(self, value):
        total = jnp.sum(jnp.where(self.is_x, value, 0.0), axis=0, keepdims=True)
        return jnp.broadcast_to(total, (8, LANES))

    def place(self, value, third, seventh):
        rest = jnp.where(self.row == 3, third, jnp.where(self.row == 7, seventh, 0.0))
        return jnp.where(self.is_xv, value, rest)

    def target(self):
        groups = []
        for group, (mine, _) in enumerate(PAIRS):
            if group < 3:
                groups.append(self.place(self.pieces[mine], 1.0, self.norm[group]))
            else:
                third = self.turn[group - 3] if self.moving else 0.0
                groups.append(self.place(self.pieces[mine], third, 0.0))
        return stack_groups(groups)

    def square(self):
        groups = []
        scaled = [jnp.where(self.is_x, -2.0 * piece, 0.0) for piece in self.pieces]
        for group, (_, theirs) in enumerate(PAIRS):
            if group < 3:
                groups.append(self.place(scaled[theirs], self.norm[group], 1.0))
            else:
                groups.append(scaled[theirs])
        return stack_groups(groups)

    def closing(self):
        groups = []
        scaled = [-4.0 * pltpu.roll(piece, 4, 0) for piece in self.pieces]
        for group, (_, theirs) in enumerate(PAIRS):
            third = self.turn[group] if group < 3 else 1.0
            groups.append(self.place(scaled[theirs], third, 0.0))
        return stack_groups(groups)

    def gather(self):
        moments = jnp.where(self.is_x, self.values * self.weight, 0.0)
        moments = jnp.where(self.row == 3, self.weight, moments)
        high, middle, low = split(moments)
        first = jnp.where(self.row < 4, high, pltpu.roll(middle, 4, 0))
        return stack_groups([first, jnp.where(self.row < 4, low, 0.0)])


def pipelined(walk, pairs, distances, work, collect, far, kept, carry):
    advance, where_is = walk

    def turn(_, carry):
        last, now = carry
        after = following(advance, advance(now[-1]), len(far))
        ahead = [distances(where_is(state)) for state in after]
        for state, force in zip(last, kept):
            collect(where_is(state), force)
        for state, block, force in zip(now, far, kept):
            work(where_is(state), block, force)
        for block, values in zip(far, ahead):
            store_all(block, values)
        return now, after

    return lax.fori_loop(0, pairs, turn, carry)


def store_all(block, values):
    for number, value in enumerate(values):
        block[number] = value


def following(advance, state, count):
    states = [state]
    while len(states) < count:
        states.append(advance(states[-1]))
    return tuple(states)


def begin(walk, state, distances, far):
    advance, where_is = walk
    now = following(advance, state, len(far))
    for block, step in zip(far, now):
        store_all(block, distances(where_is(step)))
    return now, now


def density_parts(target16, source16, weights, total_acc):
    def distances(step):
        chunk, ids = step
        mine = target16[chunk]
        return [
            jnp.dot(
                mine,
                jnp.concatenate([pick(source16, ids[2 * pair]), pick(source16, ids[2 * pair + 1])], axis=1),
                preferred_element_type=F32,
            )
            for pair in range(UNROLL // 2)
        ]

    def add(step, far, _):
        chunk, ids = step
        mass = [pick_row(weights, tile) for tile in ids]
        for group in range(LANES // 8):
            rows = slice(group * 8, group * 8 + 8)
            acc = total_acc[chunk, rows, :]
            for number in range(UNROLL):
                lanes = slice((number % 2) * LANES, (number % 2 + 1) * LANES)
                square = jnp.maximum(far[number // 2, rows, lanes], TINY)
                radius = square * lax.rsqrt(square)
                rest = 1.0 - radius
                near = 0.5 - 3.0 * (square * rest)
                clipped = jnp.maximum(rest, 0.0)
                value = jnp.minimum(near, clipped * clipped * clipped)
                acc = acc + value * mass[number]
            total_acc[chunk, rows, :] = acc

    def collect(step, kept):
        pass

    return distances, add, collect


def density_rows(total_acc, chunk):
    return (2.0 * SIGMA) * jnp.sum(total_acc[chunk].T, axis=0, keepdims=True)


def force_parts(target16, source16, gather16, sound, rho, press, mine, total_acc):
    def distances(step):
        chunk, ids = step
        return [
            jnp.dot(target16[chunk], pick(source16, tile), preferred_element_type=F32)
            for tile in ids
        ]

    def forces(step, far, force):
        chunk, ids = step
        sound_j = [pick_row(sound, tile) for tile in ids]
        rho_j = [pick_row(rho, tile) for tile in ids]
        press_j = [pick_row(press, tile) for tile in ids]
        for group in range(LANES // 16):
            for number in range(UNROLL):
                parts = []
                for sub in range(2):
                    rows = slice(group * 16 + sub * 8, group * 16 + sub * 8 + 8)
                    square = jnp.maximum(far[number, rows, 0:LANES], TINY)
                    closing = jnp.minimum(far[number, rows, LANES:], 0.0)
                    inverse = lax.rsqrt(square)
                    radius = square * inverse
                    clipped = jnp.maximum(1.0 - radius, 0.0)
                    slope = jnp.maximum(
                        2.0 - 3.0 * radius, jnp.minimum(clipped * clipped * inverse, 0.5)
                    )
                    soft = square + SOFTEN
                    both_rho = mine[chunk, group * 2 + sub, 1] + rho_j[number]
                    both_sound = mine[chunk, group * 2 + sub, 0] + sound_j[number]
                    both_press = mine[chunk, group * 2 + sub, 2] + press_j[number]
                    viscous = closing * (closing - both_sound * soft)
                    viscous = viscous / (soft * soft * both_rho)
                    parts.append((both_press + viscous) * slope)
                value = jnp.concatenate(parts, axis=0)
                high = value.astype(BF16)
                rows = slice(group * 16, group * 16 + 16)
                force[number, rows, 0:LANES] = high
                force[number, rows, LANES:] = (value - high.astype(F32)).astype(BF16)

    def collect(step, force):
        chunk, ids = step
        acc = None
        for number, tile in enumerate(ids):
            part = lax.dot_general(
                force[number],
                pick(gather16, tile),
                (((1,), (1,)), ((), ())),
                preferred_element_type=F32,
            )
            acc = part if acc is None else acc + part
        total_acc[chunk] += acc

    return distances, forces, collect


def states_of(weight, density, entropy):
    active = weight > 0.0
    safe = jnp.where(active, density, 1.0)
    entropy = jnp.where(active, entropy, 1.0)
    root = jnp.exp(jnp.log(safe) * (1.0 / 3.0))
    return jnp.sqrt(GAMMA * entropy) * root, 4.0 * safe, entropy / root


def spread(ref, chunk, field, line):
    wide = jnp.broadcast_to(line, (LANES, LANES)).T
    for group in range(LANES // 8):
        ref[chunk, group, field] = wide[group * 8 : group * 8 + 8]


class Exchange:
    def __init__(self, arrays, local_sem, send_sem, recv_sem):
        self.arrays = arrays
        self.send_sem, self.recv_sem = send_sem, recv_sem
        self.local = [
            pltpu.make_async_copy(own, near.at[1:3, 1:3, 1:3], local_sem.at[number])
            for number, (own, near) in enumerate(arrays)
        ]
        self.moved = {
            axis: {
                0: lax.axis_index(axis),
                1: lax.rem(lax.axis_index(axis) + 1, lax.axis_size(axis)),
                -1: lax.rem(lax.axis_index(axis) + lax.axis_size(axis) - 1, lax.axis_size(axis)),
            }
            for axis in ("gx", "gy", "gz")
        }
        self.plane = [(dy, dz) for dz in (-1, 1) for dy in (-1, 0, 1)] + [(-1, 0), (1, 0)]
        self.count = 0

    def device(self, dx, dy, dz):
        return {
            "gx": self.moved["gx"][dx],
            "gy": self.moved["gy"][dy],
            "gz": self.moved["gz"][dz],
        }

    def greet(self):
        barrier = pltpu.get_barrier_semaphore()
        others = [(0, dy, dz) for dy, dz in self.plane] + [(-1, 0, 0), (1, 0, 0)]
        for other in others:
            pl.semaphore_signal(
                barrier,
                inc=1,
                device_id=self.device(*other),
                device_id_type=pl.DeviceIdType.MESH,
            )
        for copy in self.local:
            copy.start()

    def send(self, source, dest, other):
        copy = pltpu.make_async_remote_copy(
            src_ref=source,
            dst_ref=dest,
            send_sem=self.send_sem.at[self.count],
            recv_sem=self.recv_sem.at[self.count],
            device_id=self.device(*other),
            device_id_type=pl.DeviceIdType.MESH,
        )
        self.count += 1
        copy.start()
        return copy

    def start_plane(self):
        pl.semaphore_wait(pltpu.get_barrier_semaphore(), len(self.plane) + 2)
        taken = {-1: slice(0, 1), 0: slice(0, 2), 1: slice(1, 2)}
        landed = {-1: slice(3, 4), 0: slice(1, 3), 1: slice(0, 1)}
        self.copies = [
            self.send(
                own.at[:, taken[dy], taken[dz]], near.at[1:3, landed[dy], landed[dz]], (0, dy, dz)
            )
            for own, near in self.arrays
            for dy, dz in self.plane
        ]

    def start_gx(self):
        for copy in self.local + self.copies:
            copy.wait()
        self.copies = []
        for _, near in self.arrays:
            self.copies.append(self.send(near.at[2:3], near.at[0:1], (1, 0, 0)))
            self.copies.append(self.send(near.at[1:2], near.at[3:4], (-1, 0, 0)))

    def finish(self):
        for copy in self.copies:
            copy.wait()


def exchange_sems(arrays):
    return [
        pltpu.SemaphoreType.DMA((arrays,)),
        pltpu.SemaphoreType.DMA((10 * arrays,)),
        pltpu.SemaphoreType.DMA((10 * arrays,)),
    ]


def staged(walk, parts, distances, work, collect, far, kept, exchange):
    carry = begin(walk, (jnp.int32(0),), distances, far)
    for number, pairs in enumerate(parts):
        carry = pipelined(walk, pairs, distances, work, collect, far, kept, carry)
        (exchange.start_plane, exchange.start_gx, exchange.finish)[number]()
    return carry[0]


DENSITY_PARTS = (5, 10, 1)
FORCE_PARTS = (3, 10, 3)


def own_cell_rows(ref, number):
    return ref[number // 4, number // 2 % 2, number % 2]


def first_kernel(own_ref, near_ref, partial_ref, target16, source16, weights, far0, far1, far2, far3, total_acc, local_sem, send_sem, recv_sem):
    exchange = Exchange([(own_ref, near_ref)], local_sem, send_sem, recv_sem)
    exchange.greet()
    for number, own in enumerate(own_cells()):
        base = cell_base(jnp.int32(own))
        rows = own_cell_rows(own_ref, number)
        for half in range(2):
            chunk = 2 * number + half
            tile = Tile(tile_rows(rows, half), base, False)
            target16[chunk] = tile.target().T.astype(BF16)
            source16[chunk] = tile.square().astype(BF16)
            weights[chunk : chunk + 1, :] = tile.weight[0:1]
    target16[2 * OWN] = jnp.zeros((LANES, WIDTH), BF16)
    total_acc[...] = jnp.zeros_like(total_acc)
    parts = density_parts(target16, source16, weights, total_acc)
    staged(own_walk(), DENSITY_PARTS, *parts, (far0, far1, far2, far3), (None,) * 4, exchange)
    for chunk in range(2 * OWN):
        partial_ref[chunk : chunk + 1, :] = density_rows(total_acc, chunk)


def density_kernel(near_ref, partial_ref, target16, out_ref, own_ref, plan, source16, weights, far0, far1, far2, far3, total_acc):
    build_plan(unit_bits(near_ref), plan)
    totals = views(plan)[4]
    put_both(weights, near_ref[pl.ds(3, TILES, stride=ROWS), :])
    weights[UNITS:PADDED, :] = jnp.zeros((8, LANES), F32)

    def prepare(turn, carry):
        for tile in needed_tiles(plan, turn):
            cell = tile >> 1
            rows = near_ref[pl.ds(pl.multiple_of(cell * 8, 8), 8), :]
            square = Tile(choose_rows(rows, tile & 1), cell_base(cell), False).square()
            source16[2 * tile] = square.astype(BF16)
            source16[2 * tile + 1] = turned(square).astype(BF16)
        return carry

    lax.fori_loop(0, (totals[1] + PREPARED - 1) // PREPARED, prepare, 0)
    for number in range(2):
        source16[UNITS + number] = jnp.zeros((WIDTH, LANES), BF16)
    total_acc[...] = jnp.zeros_like(total_acc)
    walk = listed(plan)
    distances, add, collect = density_parts(target16, source16, weights, total_acc)
    carry = begin(walk, (jnp.int32(0), jnp.int32(0)), distances, (far0, far1, far2, far3))
    pipelined(
        walk, (totals[0] + 3) // 4, distances, add, collect, (far0, far1, far2, far3), (None,) * 4, carry
    )
    for number, own in enumerate(own_cells()):
        x, y, z = number // 4, number // 2 % 2, number % 2
        for half in range(2):
            chunk = 2 * number + half
            part = slice(half * LANES, (half + 1) * LANES)
            row = (2 * own + half) * ROWS + 3
            value = partial_ref[chunk : chunk + 1, :] + density_rows(total_acc, chunk)
            value = jnp.where(near_ref[row : row + 1, :] > 0.0, value, 0.0)
            out_ref[x, y, z : z + 1, part] = value
            own_ref[x, y, z, half : half + 1, :] = value


def second_kernel(place_ref, speed_ref, rho_ref, near_speed_ref, near_rho_ref, partial_ref, target16, source16, gather16, sound, rho, press, mine, far0, far1, far2, far3, force0, force1, force2, force3, total_acc, local_sem, send_sem, recv_sem):
    exchange = Exchange(
        [(speed_ref, near_speed_ref), (rho_ref, near_rho_ref)], local_sem, send_sem, recv_sem
    )
    exchange.greet()
    for number, own in enumerate(own_cells()):
        base = cell_base(jnp.int32(own))
        places = own_cell_rows(place_ref, number)
        speeds = own_cell_rows(speed_ref, number)
        density = own_cell_rows(rho_ref, number)
        for half in range(2):
            chunk = 2 * number + half
            rows = tile_rows(places, half, speeds)
            tile = Tile(rows, base, True)
            target16[chunk] = tile.target().T.astype(BF16)
            source16[chunk, :, 0:LANES] = tile.square().astype(BF16)
            source16[chunk, :, LANES:] = tile.closing().astype(BF16)
            masses = tile.gather().astype(BF16)
            gather16[chunk, :, 0:LANES] = masses
            gather16[chunk, :, LANES:] = masses
            states = states_of(rows[3:4], density[half : half + 1], rows[7:8])
            for field, (value, far) in enumerate(zip(states, (sound, rho, press))):
                far[chunk : chunk + 1, :] = value
                spread(mine, chunk, field, value)
    target16[2 * OWN] = jnp.zeros((LANES, WIDTH), BF16)
    total_acc[...] = jnp.zeros_like(total_acc)
    for ref in (force0, force1, force2, force3):
        ref[...] = jnp.zeros_like(ref)
    parts = force_parts(
        target16, source16, gather16, sound, rho, press, mine, total_acc
    )
    walk = own_walk()
    last = staged(walk, FORCE_PARTS, *parts, (far0, far1, far2, far3), (force0, force1, force2, force3), exchange)
    for state, force in zip(last, (force0, force1, force2, force3)):
        parts[2](walk[1](state), force)
    for chunk in range(2 * OWN):
        partial_ref[chunk] = total_acc[chunk].T


def force_kernel(plan, near_ref, speed_ref, rho_ref, partial_ref, target16, out_ref, source16, gather16, sound, rho, press, mine, far0, far1, far2, far3, force0, force1, force2, force3, total_acc):
    totals = views(plan)[4]
    states = states_of(
        near_ref[pl.ds(3, TILES, stride=ROWS), :],
        rho_ref[...],
        speed_ref[pl.ds(3, TILES, stride=ROWS), :],
    )
    for value, ref in zip(states, (sound, rho, press)):
        put_both(ref, value)
        ref[UNITS:PADDED, :] = jnp.ones((8, LANES), F32)

    def prepare(turn, carry):
        for number in needed_tiles(plan, turn):
            cell = number >> 1
            place = pl.ds(pl.multiple_of(cell * 8, 8), 8)
            rows = choose_rows(near_ref[place, :], number & 1, speed_ref[place, :])
            tile = Tile(rows, cell_base(cell), True)
            square, closing, masses = tile.square(), tile.closing(), tile.gather()
            for unit in (2 * number, 2 * number + 1):
                source16[unit, :, 0:LANES] = square.astype(BF16)
                source16[unit, :, LANES:] = closing.astype(BF16)
                gather16[unit, :, 0:LANES] = masses.astype(BF16)
                gather16[unit, :, LANES:] = masses.astype(BF16)
                square, closing, masses = turned(square), turned(closing), turned(masses)
        return carry

    lax.fori_loop(0, (totals[1] + PREPARED - 1) // PREPARED, prepare, 0)
    for number in range(2):
        source16[UNITS + number] = jnp.zeros((WIDTH, 2 * LANES), BF16)
        gather16[UNITS + number] = jnp.zeros((16, 2 * LANES), BF16)
    for number, own in enumerate(own_cells()):
        for half in range(2):
            line = slice(4 * own + 2 * half, 4 * own + 2 * half + 1)
            for field, ref in enumerate((sound, rho, press)):
                spread(mine, 2 * number + half, field, ref[line, :])
    mine[2 * OWN] = jnp.ones((LANES // 8, 3, 8, LANES), F32)
    total_acc[...] = jnp.zeros_like(total_acc)
    for ref in (force0, force1, force2, force3):
        ref[...] = jnp.zeros_like(ref)
    walk = listed(plan)
    distances, forces, collect = force_parts(
        target16, source16, gather16, sound, rho, press, mine, total_acc
    )
    carry = begin(walk, (jnp.int32(0), jnp.int32(0)), distances, (far0, far1, far2, far3))
    last, _ = pipelined(
        walk,
        (totals[0] + 3) // 4,
        distances,
        forces,
        collect,
        (far0, far1, far2, far3),
        (force0, force1, force2, force3),
        carry,
    )
    for state, force in zip(last, (force0, force1, force2, force3)):
        collect(walk[1](state), force)
    for number, own in enumerate(own_cells()):
        x, y, z = number // 4, number // 2 % 2, number % 2
        for half in range(2):
            chunk = 2 * number + half
            sums = total_acc[chunk].T + partial_ref[chunk]
            sums = sums[0:4] + sums[4:8] + sums[8:12]
            top = (2 * own + half) * ROWS
            shown = near_ref[top + 3 : top + 4, :] > 0.0
            part = slice(half * LANES, (half + 1) * LANES)
            for axis in range(3):
                offset = float((own // 16, own // 4 % 4, own % 4)[axis] - 2)
                place = near_ref[top + axis : top + axis + 1, :] + offset
                value = (-6.0 * SIGMA) * (sums[axis : axis + 1] - place * sums[3:4])
                out_ref[axis, x, y, z : z + 1, part] = jnp.where(shown, value, 0.0)


def vmem(number):
    return [pl.BlockSpec(memory_space=pltpu.VMEM) for _ in range(number)]


def smem():
    return pl.BlockSpec(memory_space=pltpu.SMEM)


CELL_BLOCK = (2 * ROWS, LANES)
NEAR = (WIDE, WIDE, WIDE)
TARGETS = jax.ShapeDtypeStruct((2 * OWN + 1, LANES, WIDTH), BF16)


def first_call(own):
    return pl.pallas_call(
        first_kernel,
        out_shape=(
            jax.ShapeDtypeStruct(NEAR + CELL_BLOCK, F32),
            jax.ShapeDtypeStruct((2 * OWN, LANES), F32),
            TARGETS,
        ),
        in_specs=vmem(1),
        out_specs=tuple(vmem(3)),
        scratch_shapes=[
            pltpu.VMEM((2 * OWN, WIDTH, LANES), BF16),
            pltpu.VMEM((2 * OWN, LANES), F32),
            pltpu.VMEM((UNROLL // 2, LANES, 2 * LANES), F32),
            pltpu.VMEM((UNROLL // 2, LANES, 2 * LANES), F32),
            pltpu.VMEM((UNROLL // 2, LANES, 2 * LANES), F32),
            pltpu.VMEM((UNROLL // 2, LANES, 2 * LANES), F32),
            pltpu.VMEM((2 * OWN + 1, LANES, LANES), F32),
        ]
        + exchange_sems(1),
        compiler_params=pltpu.CompilerParams(collective_id=0, has_side_effects=True),
        name="first",
    )(own)


def density_call(near, partial, targets):
    return pl.pallas_call(
        density_kernel,
        out_shape=(
            jax.ShapeDtypeStruct((2, 2, 2, SLOTS), F32),
            jax.ShapeDtypeStruct((2, 2, 2, 2, LANES), F32),
            jax.ShapeDtypeStruct((PLAN,), jnp.int32),
        ),
        in_specs=vmem(3),
        out_specs=tuple(vmem(2) + [smem()]),
        scratch_shapes=[
            pltpu.VMEM((UNITS + 2, WIDTH, LANES), BF16),
            pltpu.VMEM((PADDED, LANES), F32),
            pltpu.VMEM((UNROLL // 2, LANES, 2 * LANES), F32),
            pltpu.VMEM((UNROLL // 2, LANES, 2 * LANES), F32),
            pltpu.VMEM((UNROLL // 2, LANES, 2 * LANES), F32),
            pltpu.VMEM((UNROLL // 2, LANES, 2 * LANES), F32),
            pltpu.VMEM((2 * OWN + 1, LANES, LANES), F32),
        ],
        name="density",
    )(near, partial, targets)


def force_scratch(tiles, padded):
    return [
        pltpu.VMEM((tiles, WIDTH, 2 * LANES), BF16),
        pltpu.VMEM((tiles, 16, 2 * LANES), BF16),
        pltpu.VMEM((padded, LANES), F32),
        pltpu.VMEM((padded, LANES), F32),
        pltpu.VMEM((padded, LANES), F32),
        pltpu.VMEM((2 * OWN + 1, LANES // 8, 3, 8, LANES), F32),
        pltpu.VMEM((UNROLL, LANES, 2 * LANES), F32),
        pltpu.VMEM((UNROLL, LANES, 2 * LANES), F32),
        pltpu.VMEM((UNROLL, LANES, 2 * LANES), F32),
        pltpu.VMEM((UNROLL, LANES, 2 * LANES), F32),
        pltpu.VMEM((UNROLL, LANES, 2 * LANES), BF16),
        pltpu.VMEM((UNROLL, LANES, 2 * LANES), BF16),
        pltpu.VMEM((UNROLL, LANES, 2 * LANES), BF16),
        pltpu.VMEM((UNROLL, LANES, 2 * LANES), BF16),
        pltpu.VMEM((2 * OWN + 1, LANES, 16), F32),
    ]


def second_call(place, speed, rho):
    return pl.pallas_call(
        second_kernel,
        out_shape=(
            jax.ShapeDtypeStruct(NEAR + CELL_BLOCK, F32),
            jax.ShapeDtypeStruct(NEAR + (2, LANES), F32),
            jax.ShapeDtypeStruct((2 * OWN, 16, LANES), F32),
            TARGETS,
        ),
        in_specs=vmem(3),
        out_specs=tuple(vmem(4)),
        scratch_shapes=force_scratch(2 * OWN, 2 * OWN) + exchange_sems(2),
        compiler_params=pltpu.CompilerParams(collective_id=1, has_side_effects=True),
        name="second",
    )(place, speed, rho)


def force_call(plan, near, speed, rho, partial, targets):
    return pl.pallas_call(
        force_kernel,
        out_shape=jax.ShapeDtypeStruct((3, 2, 2, 2, SLOTS), F32),
        in_specs=[smem()] + vmem(5),
        out_specs=vmem(1)[0],
        scratch_shapes=force_scratch(UNITS + 2, PADDED),
        name="force",
    )(plan, near, speed, rho, partial, targets)


def per_device(positions, velocities, masses, entropy, counts):
    slot_ids = lax.broadcasted_iota(jnp.int32, masses.shape, 3)
    weight = jnp.where(slot_ids < counts[..., None], masses, 0.0)
    halves = masses.shape[:3] + (2, LANES)

    def blocks(parts):
        joined = jnp.stack([part.reshape(halves) for part in parts], axis=4)
        return joined.reshape(masses.shape[:3] + CELL_BLOCK)

    place = blocks([positions[0], positions[1], positions[2], weight])
    speed = blocks([velocities[0], velocities[1], velocities[2], entropy])
    near, partial, targets = first_call(place)
    near = near.reshape(CELLS * 8, LANES)
    density, own_rho, plan = density_call(near, partial, targets)
    near_speed, near_rho, sums, targets = second_call(place, speed, own_rho)
    near_speed = near_speed.reshape(CELLS * 8, LANES)
    accel = force_call(plan, near, near_speed, near_rho.reshape(TILES, LANES), sums, targets)
    return density, accel


def solution(mesh):
    return jax.shard_map(
        per_device,
        mesh=mesh,
        in_specs=(
            P(None, "gx", "gy", "gz", None),
            P(None, "gx", "gy", "gz", None),
            P("gx", "gy", "gz", None),
            P("gx", "gy", "gz", None),
            P("gx", "gy", "gz"),
        ),
        out_specs=(P("gx", "gy", "gz", None), P(None, "gx", "gy", "gz", None)),
        check_vma=False,
    )
```

```python
import functools
import math

import jax
import jax.numpy as jnp
from jax import lax
from jax.experimental import pallas as pl
from jax.experimental.pallas import tpu as pltpu
from jax.sharding import PartitionSpec as P

SIGMA = 8.0 / math.pi
GAMMA = 5.0 / 3.0
SOFTEN = 0.01
TINY = 1e-12
SLOTS = 256
WIDE = 4
CELLS = WIDE * WIDE * WIDE
OWN = 8
LANES = 128
TILES = 2 * CELLS
UNITS = 2 * TILES
UNROLL = 2
TURN = 8
OWN_UNROLL = 4
OWN_TURN = 4
LIST = 128
ORDER_AT = 9 * LIST
COUNT_AT = ORDER_AT + 24
NEEDED_AT = COUNT_AT + 24
TOTAL_AT = NEEDED_AT + 144
PLAN = 11 * LIST
PREPARED = 4
CHUNK_STEPS = 2 * OWN // OWN_UNROLL
OWN_STEPS = 2 * OWN * CHUNK_STEPS
HALF = LANES // 2
ROWS = 4
GROUPS = 6
WIDTH = 8 * GROUPS
PADDED = UNITS + 8
F32 = jnp.float32
BF16 = jnp.bfloat16


def cell_id(x, y, z):
    return (x * WIDE + y) * WIDE + z


def own_cells():
    return [cell_id(1 + n // 4, 1 + n // 2 % 2, 1 + n % 2) for n in range(OWN)]


def halo_neighbours(number):
    x, y, z = 1 + number // 4, 1 + number // 2 % 2, 1 + number % 2
    around = [
        cell_id(x + dx, y + dy, z + dz)
        for dx in (-1, 0, 1)
        for dy in (-1, 0, 1)
        for dz in (-1, 0, 1)
    ]
    return [other for other in around if other not in own_cells()]


def unit_bits(near_ref):
    lower = near_ref[pl.ds(ROWS - 1, CELLS, stride=2 * ROWS), :]
    upper = near_ref[pl.ds(2 * ROWS - 1, CELLS, stride=2 * ROWS), :]
    ids = lax.broadcasted_iota(jnp.int32, (8, LANES), 0)
    lanes = lax.broadcasted_iota(jnp.int32, (8, LANES), 1)
    power = jnp.ones((8, LANES), F32)
    for bit in range(3):
        power = jnp.where((ids & (1 << bit)) > 0, power * float(4 ** (1 << bit)), power)
    bits = []
    for group in range(CELLS // 8):
        part = slice(8 * group, 8 * group + 8)
        middle = lanes == HALF
        value = jnp.where(middle & (lower[part] > 0.0), power, 0.0)
        value = value + jnp.where((middle | (lanes == 0)) & (upper[part] > 0.0), power, 0.0)
        bits.append(jnp.sum(value).astype(jnp.int32))

    def extra_of(cell):
        return (bits[cell // 8] >> (2 * (cell % 8))) & 3

    return extra_of


class View:
    def __init__(self, plan, base):
        self.plan, self.base = plan, base

    def __getitem__(self, index):
        return self.plan[self.base + index]

    def __setitem__(self, index, value):
        self.plan[self.base + index] = value


def views(plan):
    return [View(plan, base) for base in (0, ORDER_AT, COUNT_AT, NEEDED_AT, TOTAL_AT)]


def build_plan(extra_of, plan):
    tiles, order, count_of, needed, totals = views(plan)
    used = jnp.int32(0)
    for cell in range(CELLS):
        if cell in own_cells():
            continue
        needed[used] = jnp.int32(2 * cell)
        needed[used + 1] = jnp.int32(2 * cell + 1)
        used = used + 1 + (extra_of(cell) >> 1)
    for extra in range(PREPARED - 1):
        needed[used + extra] = jnp.int32(0)
    totals[1] = used
    total = jnp.int32(0)
    place = jnp.int32(0)
    for number, own in enumerate(own_cells()):
        where = jnp.int32(number * LIST)
        for other in halo_neighbours(number):
            for unit in range(4):
                tiles[where + unit] = jnp.int32(4 * other + unit)
            where = where + 1 + extra_of(other)
        for extra in range(2 * UNROLL - 1):
            tiles[where + extra] = jnp.int32(UNITS)
        count = (where - number * LIST + 2 * UNROLL - 1) // (2 * UNROLL)
        for half in range(2):
            order[place] = jnp.int32(2 * number + half)
            count_of[place] = count
            used = 1 if half == 0 else extra_of(own) >> 1
            place = place + used
            total = total + used * count
    order[place] = jnp.int32(2 * OWN)
    count_of[place] = jnp.int32(1 << 20)
    for extra in range(LIST):
        tiles[OWN * LIST + extra] = jnp.int32(UNITS)
    totals[0] = total


def listed(plan):
    tiles, order, count_of, _, _ = views(plan)

    def advance(state):
        place, step = state
        more = step + 1 < count_of[place]
        return jnp.where(more, place, place + 1), jnp.where(more, step + 1, 0)

    def where_is(state):
        chunk = order[state[0]]
        start = (chunk >> 1) * LIST + state[1] * (2 * UNROLL)
        units = [tiles[start + number] for number in range(2 * UNROLL)]
        return chunk, [(units[2 * n], units[2 * n + 1] ^ 1) for n in range(UNROLL)]

    return advance, where_is


def pick(ref, tile):
    if not isinstance(tile, tuple):
        return ref[tile]
    low, high = tile
    lanes = lax.broadcasted_iota(jnp.int32, ref.shape[1:], 1)
    return jnp.where((lanes & HALF) == 0, ref[low], ref[high])


def pick_row(ref, tile):
    if not isinstance(tile, tuple):
        return ref[pl.ds(tile, 1), :]
    low, high = tile
    lanes = lax.broadcasted_iota(jnp.int32, (1, LANES), 1)
    return jnp.where((lanes & HALF) == 0, ref[pl.ds(low, 1), :], ref[pl.ds(high, 1), :])


def turned(value):
    return pltpu.roll(value, HALF, 1)


def put_both(ref, value):
    ref[pl.ds(0, TILES, stride=2), :] = value
    ref[pl.ds(1, TILES, stride=2), :] = turned(value)


def own_walk():
    def advance(state):
        return (jnp.minimum(state[0] + 1, OWN_STEPS - 1),)

    def where_is(state):
        first = (state[0] % CHUNK_STEPS) * OWN_UNROLL
        return state[0] // CHUNK_STEPS, [first + number for number in range(OWN_UNROLL)]

    return advance, where_is


def split(value):
    high = value.astype(BF16).astype(F32)
    rest = value - high
    middle = rest.astype(BF16).astype(F32)
    low = rest - middle
    return high, middle, low


PAIRS = ((0, 0), (0, 1), (1, 0), (1, 1), (0, 2), (2, 0))


def needed_tiles(plan, turn):
    needed = views(plan)[3]
    return [needed[turn * PREPARED + number] for number in range(PREPARED)]


def choose_rows(place, half, speed=None):
    other = pltpu.roll(place, 4, 0)
    row = lax.broadcasted_iota(jnp.int32, (8, LANES), 0)
    place = jnp.where(half > 0, other, place)
    if speed is None:
        return jnp.where(row < 4, place, 0.0)
    return jnp.where(row < 4, place, jnp.where(half > 0, speed, pltpu.roll(speed, 4, 0)))


def tile_rows(place, half, speed=None):
    if half:
        place = pltpu.roll(place, 4, 0)
    elif speed is not None:
        speed = pltpu.roll(speed, 4, 0)
    row = lax.broadcasted_iota(jnp.int32, (8, LANES), 0)
    return jnp.where(row < 4, place, 0.0 if speed is None else speed)


def cell_base(cell):
    row = lax.broadcasted_iota(jnp.int32, (8, LANES), 0)
    x, y, z = [
        (value - 2).astype(F32) for value in (cell >> 4, (cell >> 2) & 3, cell & 3)
    ]
    return jnp.where(row == 0, x, jnp.where(row == 1, y, jnp.where(row == 2, z, 0.0)))


def stack_groups(groups):
    return jnp.concatenate(groups, axis=0)


class Tile:
    def __init__(self, rows, base, moving):
        row = lax.broadcasted_iota(jnp.int32, (8, LANES), 0)
        self.moving = moving
        self.row = row
        self.is_x = row < 3
        self.is_xv = (row < 3) | ((row >= 4) & (row < 7))
        self.weight = jnp.broadcast_to(rows[3:4], (8, LANES))
        self.values = jnp.where((self.weight > 0.0) & self.is_xv, rows + base, 0.0)
        self.pieces = split(self.values)
        squares = self.values * self.values
        self.norm = split(self.fold(squares))
        if moving:
            self.turn = split(4.0 * self.fold(self.values * pltpu.roll(self.values, 4, 0)))

    def fold(self, value):
        total = jnp.sum(jnp.where(self.is_x, value, 0.0), axis=0, keepdims=True)
        return jnp.broadcast_to(total, (8, LANES))

    def place(self, value, third, seventh):
        rest = jnp.where(self.row == 3, third, jnp.where(self.row == 7, seventh, 0.0))
        return jnp.where(self.is_xv, value, rest)

    def target(self):
        groups = []
        for group, (mine, _) in enumerate(PAIRS):
            if group < 3:
                groups.append(self.place(self.pieces[mine], 1.0, self.norm[group]))
            else:
                third = self.turn[group - 3] if self.moving else 0.0
                groups.append(self.place(self.pieces[mine], third, 0.0))
        return stack_groups(groups)

    def square(self):
        groups = []
        scaled = [jnp.where(self.is_x, -2.0 * piece, 0.0) for piece in self.pieces]
        for group, (_, theirs) in enumerate(PAIRS):
            if group < 3:
                groups.append(self.place(scaled[theirs], self.norm[group], 1.0))
            else:
                groups.append(scaled[theirs])
        return stack_groups(groups)

    def closing(self):
        groups = []
        scaled = [-4.0 * pltpu.roll(piece, 4, 0) for piece in self.pieces]
        for group, (_, theirs) in enumerate(PAIRS):
            third = self.turn[group] if group < 3 else 1.0
            groups.append(self.place(scaled[theirs], third, 0.0))
        return stack_groups(groups)

    def gather(self):
        moments = jnp.where(self.is_x, self.values * self.weight, 0.0)
        moments = jnp.where(self.row == 3, self.weight, moments)
        high, middle, low = split(moments)
        first = jnp.where(self.row < 4, high, pltpu.roll(middle, 4, 0))
        return stack_groups([first, jnp.where(self.row < 4, low, 0.0)])


def pipelined(walk, pairs, distances, work, collect, far, kept, carry):
    advance, where_is = walk

    def turn(_, carry):
        last, now = carry
        after = following(advance, advance(now[-1]), len(far))
        ahead = [distances(where_is(state)) for state in after]
        for state, force in zip(last, kept):
            collect(where_is(state), force)
        for state, block, force in zip(now, far, kept):
            work(where_is(state), block, force)
        for block, values in zip(far, ahead):
            store_all(block, values)
        return now, after

    return lax.fori_loop(0, pairs, turn, carry)


def store_all(block, values):
    for number, value in enumerate(values):
        block[number] = value


def following(advance, state, count):
    states = [state]
    while len(states) < count:
        states.append(advance(states[-1]))
    return tuple(states)


def begin(walk, state, distances, far):
    advance, where_is = walk
    now = following(advance, state, len(far))
    for block, step in zip(far, now):
        store_all(block, distances(where_is(step)))
    return now, now


def density_parts(unroll, target16, source16, weights, total_acc):
    def distances(step):
        chunk, ids = step
        mine = target16[chunk]
        return [
            jnp.dot(
                mine,
                jnp.concatenate([pick(source16, ids[2 * pair]), pick(source16, ids[2 * pair + 1])], axis=1),
                preferred_element_type=F32,
            )
            for pair in range(unroll // 2)
        ]

    def add(step, far, _):
        chunk, ids = step
        mass = [pick_row(weights, tile) for tile in ids]
        for group in range(LANES // 8):
            rows = slice(group * 8, group * 8 + 8)
            acc = total_acc[chunk, rows, :]
            for number in range(unroll):
                lanes = slice((number % 2) * LANES, (number % 2 + 1) * LANES)
                square = jnp.maximum(far[number // 2, rows, lanes], TINY)
                radius = square * lax.rsqrt(square)
                rest = 1.0 - radius
                near = 0.5 - 3.0 * (square * rest)
                clipped = jnp.maximum(rest, 0.0)
                value = jnp.minimum(near, clipped * clipped * clipped)
                acc = acc + value * mass[number]
            total_acc[chunk, rows, :] = acc

    def collect(step, kept):
        pass

    return distances, add, collect


def density_rows(total_acc, chunk):
    return (2.0 * SIGMA) * jnp.sum(total_acc[chunk].T, axis=0, keepdims=True)


def force_parts(unroll, target16, source16, gather16, sound, rho, press, mine, total_acc):
    def distances(step):
        chunk, ids = step
        return [
            jnp.dot(target16[chunk], pick(source16, tile), preferred_element_type=F32)
            for tile in ids
        ]

    def forces(step, far, force):
        chunk, ids = step
        sound_j = [pick_row(sound, tile) for tile in ids]
        rho_j = [pick_row(rho, tile) for tile in ids]
        press_j = [pick_row(press, tile) for tile in ids]
        for group in range(LANES // 16):
            for number in range(unroll):
                parts = []
                for sub in range(2):
                    rows = slice(group * 16 + sub * 8, group * 16 + sub * 8 + 8)
                    square = jnp.minimum(jnp.maximum(far[number, rows, 0:LANES], TINY), 1.0)
                    closing = jnp.minimum(far[number, rows, LANES:], 0.0)
                    inverse = lax.rsqrt(square)
                    radius = square * inverse
                    slope = jnp.maximum(
                        4.0 - 3.0 * radius, jnp.minimum(inverse + radius, 2.5)
                    )
                    slope = slope - 2.0
                    approach = closing / (square + SOFTEN)
                    both_rho = mine[chunk, group * 2 + sub, 1] + rho_j[number]
                    both_sound = mine[chunk, group * 2 + sub, 0] + sound_j[number]
                    both_press = mine[chunk, group * 2 + sub, 2] + press_j[number]
                    viscous = approach * (approach - both_sound) / both_rho
                    parts.append((both_press + viscous) * slope)
                value = jnp.concatenate(parts, axis=0)
                rows = slice(group * 16, group * 16 + 16)
                force[number, rows, 0:LANES] = value
                force[number, rows, LANES:] = value - value.astype(BF16).astype(F32)

    def collect(step, force):
        chunk, ids = step
        acc = None
        for number, tile in enumerate(ids):
            part = lax.dot_general(
                force[number],
                pick(gather16, tile),
                (((1,), (1,)), ((), ())),
                preferred_element_type=F32,
            )
            acc = part if acc is None else acc + part
        total_acc[chunk] += acc

    return distances, forces, collect


def states_of(weight, density, entropy):
    active = weight > 0.0
    safe = jnp.where(active, density, 1.0)
    entropy = jnp.where(active, entropy, 1.0)
    root = jnp.exp(jnp.log(safe) * (1.0 / 3.0))
    return jnp.sqrt(GAMMA * entropy) * root, 4.0 * safe, entropy / root


def spread(ref, chunk, field, line):
    wide = jnp.broadcast_to(line, (LANES, LANES)).T
    for group in range(LANES // 8):
        ref[chunk, group, field] = wide[group * 8 : group * 8 + 8]


class Exchange:
    def __init__(self, arrays, local_sem, send_sem, recv_sem):
        self.arrays = arrays
        self.send_sem, self.recv_sem = send_sem, recv_sem
        self.local = [
            pltpu.make_async_copy(own, near.at[1:3, 1:3, 1:3], local_sem.at[number])
            for number, (own, near) in enumerate(arrays)
        ]
        self.moved = {
            axis: {
                0: lax.axis_index(axis),
                1: lax.rem(lax.axis_index(axis) + 1, lax.axis_size(axis)),
                -1: lax.rem(lax.axis_index(axis) + lax.axis_size(axis) - 1, lax.axis_size(axis)),
            }
            for axis in ("gx", "gy", "gz")
        }
        self.plane = [(dy, dz) for dz in (-1, 1) for dy in (-1, 0, 1)] + [(-1, 0), (1, 0)]
        self.count = 0

    def device(self, dx, dy, dz):
        return {
            "gx": self.moved["gx"][dx],
            "gy": self.moved["gy"][dy],
            "gz": self.moved["gz"][dz],
        }

    def greet(self):
        barrier = pltpu.get_barrier_semaphore()
        others = [(0, dy, dz) for dy, dz in self.plane] + [(-1, 0, 0), (1, 0, 0)]
        for other in others:
            pl.semaphore_signal(
                barrier,
                inc=1,
                device_id=self.device(*other),
                device_id_type=pl.DeviceIdType.MESH,
            )
        for copy in self.local:
            copy.start()

    def send(self, source, dest, other):
        copy = pltpu.make_async_remote_copy(
            src_ref=source,
            dst_ref=dest,
            send_sem=self.send_sem.at[self.count],
            recv_sem=self.recv_sem.at[self.count],
            device_id=self.device(*other),
            device_id_type=pl.DeviceIdType.MESH,
        )
        self.count += 1
        copy.start()
        return copy

    def start_plane(self):
        pl.semaphore_wait(pltpu.get_barrier_semaphore(), len(self.plane) + 2)
        taken = {-1: slice(0, 1), 0: slice(0, 2), 1: slice(1, 2)}
        landed = {-1: slice(3, 4), 0: slice(1, 3), 1: slice(0, 1)}
        self.copies = [
            self.send(
                own.at[:, taken[dy], taken[dz]], near.at[1:3, landed[dy], landed[dz]], (0, dy, dz)
            )
            for own, near in self.arrays
            for dy, dz in self.plane
        ]

    def start_gx(self):
        for copy in self.local + self.copies:
            copy.wait()
        self.copies = []
        for _, near in self.arrays:
            self.copies.append(self.send(near.at[2:3], near.at[0:1], (1, 0, 0)))
            self.copies.append(self.send(near.at[1:2], near.at[3:4], (-1, 0, 0)))

    def finish(self):
        for copy in self.copies:
            copy.wait()


def exchange_sems(arrays):
    return [
        pltpu.SemaphoreType.DMA((arrays,)),
        pltpu.SemaphoreType.DMA((10 * arrays,)),
        pltpu.SemaphoreType.DMA((10 * arrays,)),
    ]


def staged(walk, parts, distances, work, collect, far, kept, exchange):
    carry = begin(walk, (jnp.int32(0),), distances, far)
    for number, pairs in enumerate(parts):
        carry = pipelined(walk, pairs, distances, work, collect, far, kept, carry)
        (exchange.start_plane, exchange.start_gx, exchange.finish)[number]()
    return carry[0]


DENSITY_PARTS = (5, 10, 1)
FORCE_PARTS = (3, 10, 3)


def own_cell_rows(ref, number):
    return ref[number // 4, number // 2 % 2, number % 2]


def first_kernel(own_ref, near_ref, partial_ref, target16, source16, weights, far0, far1, far2, far3, total_acc, local_sem, send_sem, recv_sem):
    exchange = Exchange([(own_ref, near_ref)], local_sem, send_sem, recv_sem)
    exchange.greet()
    for number, own in enumerate(own_cells()):
        base = cell_base(jnp.int32(own))
        rows = own_cell_rows(own_ref, number)
        for half in range(2):
            chunk = 2 * number + half
            tile = Tile(tile_rows(rows, half), base, False)
            target16[chunk] = tile.target().T.astype(BF16)
            source16[chunk] = tile.square().astype(BF16)
            weights[chunk : chunk + 1, :] = tile.weight[0:1]
    target16[2 * OWN] = jnp.zeros((LANES, WIDTH), BF16)
    total_acc[...] = jnp.zeros_like(total_acc)
    parts = density_parts(OWN_UNROLL, target16, source16, weights, total_acc)
    staged(own_walk(), DENSITY_PARTS, *parts, (far0, far1, far2, far3), (None,) * OWN_TURN, exchange)
    for chunk in range(2 * OWN):
        partial_ref[chunk : chunk + 1, :] = density_rows(total_acc, chunk)


def density_kernel(near_ref, partial_ref, target16, out_ref, own_ref, plan, source16, weights, far0, far1, far2, far3, far4, far5, far6, far7, total_acc):
    build_plan(unit_bits(near_ref), plan)
    totals = views(plan)[4]
    put_both(weights, near_ref[pl.ds(3, TILES, stride=ROWS), :])
    weights[UNITS:PADDED, :] = jnp.zeros((8, LANES), F32)

    def prepare(turn, carry):
        for tile in needed_tiles(plan, turn):
            cell = tile >> 1
            rows = near_ref[pl.ds(pl.multiple_of(cell * 8, 8), 8), :]
            square = Tile(choose_rows(rows, tile & 1), cell_base(cell), False).square()
            source16[2 * tile] = square.astype(BF16)
            source16[2 * tile + 1] = turned(square).astype(BF16)
        return carry

    lax.fori_loop(0, (totals[1] + PREPARED - 1) // PREPARED, prepare, 0)
    for number in range(2):
        source16[UNITS + number] = jnp.zeros((WIDTH, LANES), BF16)
    total_acc[...] = jnp.zeros_like(total_acc)
    walk = listed(plan)
    distances, add, collect = density_parts(UNROLL, target16, source16, weights, total_acc)
    carry = begin(walk, (jnp.int32(0), jnp.int32(0)), distances, (far0, far1, far2, far3, far4, far5, far6, far7))
    pipelined(
        walk, (totals[0] + TURN - 1) // TURN, distances, add, collect, (far0, far1, far2, far3, far4, far5, far6, far7), (None,) * TURN, carry
    )
    for number, own in enumerate(own_cells()):
        x, y, z = number // 4, number // 2 % 2, number % 2
        for half in range(2):
            chunk = 2 * number + half
            part = slice(half * LANES, (half + 1) * LANES)
            row = (2 * own + half) * ROWS + 3
            value = partial_ref[chunk : chunk + 1, :] + density_rows(total_acc, chunk)
            value = jnp.where(near_ref[row : row + 1, :] > 0.0, value, 0.0)
            out_ref[x, y, z : z + 1, part] = value
            own_ref[x, y, z, half : half + 1, :] = value


def second_kernel(place_ref, speed_ref, rho_ref, near_speed_ref, near_rho_ref, partial_ref, target16, source16, gather16, sound, rho, press, mine, far0, far1, far2, far3, force0, force1, force2, force3, total_acc, local_sem, send_sem, recv_sem):
    exchange = Exchange(
        [(speed_ref, near_speed_ref), (rho_ref, near_rho_ref)], local_sem, send_sem, recv_sem
    )
    exchange.greet()
    for number, own in enumerate(own_cells()):
        base = cell_base(jnp.int32(own))
        places = own_cell_rows(place_ref, number)
        speeds = own_cell_rows(speed_ref, number)
        density = own_cell_rows(rho_ref, number)
        for half in range(2):
            chunk = 2 * number + half
            rows = tile_rows(places, half, speeds)
            tile = Tile(rows, base, True)
            target16[chunk] = tile.target().T.astype(BF16)
            source16[chunk, :, 0:LANES] = tile.square().astype(BF16)
            source16[chunk, :, LANES:] = tile.closing().astype(BF16)
            masses = tile.gather()
            gather16[chunk, :, 0:LANES] = masses
            gather16[chunk, :, LANES:] = masses
            states = states_of(rows[3:4], density[half : half + 1], rows[7:8])
            for field, (value, far) in enumerate(zip(states, (sound, rho, press))):
                far[chunk : chunk + 1, :] = value
                spread(mine, chunk, field, value)
    target16[2 * OWN] = jnp.zeros((LANES, WIDTH), BF16)
    total_acc[...] = jnp.zeros_like(total_acc)
    for ref in (force0, force1, force2, force3):
        ref[...] = jnp.zeros_like(ref)
    parts = force_parts(
        OWN_UNROLL, target16, source16, gather16, sound, rho, press, mine, total_acc
    )
    walk = own_walk()
    last = staged(walk, FORCE_PARTS, *parts, (far0, far1, far2, far3), (force0, force1, force2, force3), exchange)
    for state, force in zip(last, (force0, force1, force2, force3)):
        parts[2](walk[1](state), force)
    for chunk in range(2 * OWN):
        partial_ref[chunk] = total_acc[chunk].T


def force_kernel(plan, near_ref, speed_ref, rho_ref, partial_ref, target16, out_ref, source16, gather16, sound, rho, press, mine, far0, far1, far2, far3, far4, far5, far6, far7, force0, force1, force2, force3, force4, force5, force6, force7, total_acc):
    totals = views(plan)[4]
    states = states_of(
        near_ref[pl.ds(3, TILES, stride=ROWS), :],
        rho_ref[...],
        speed_ref[pl.ds(3, TILES, stride=ROWS), :],
    )
    for value, ref in zip(states, (sound, rho, press)):
        put_both(ref, value)
        ref[UNITS:PADDED, :] = jnp.ones((8, LANES), F32)

    def prepare(turn, carry):
        for number in needed_tiles(plan, turn):
            cell = number >> 1
            place = pl.ds(pl.multiple_of(cell * 8, 8), 8)
            rows = choose_rows(near_ref[place, :], number & 1, speed_ref[place, :])
            tile = Tile(rows, cell_base(cell), True)
            square, closing, masses = tile.square(), tile.closing(), tile.gather()
            for unit in (2 * number, 2 * number + 1):
                source16[unit, :, 0:LANES] = square.astype(BF16)
                source16[unit, :, LANES:] = closing.astype(BF16)
                gather16[unit, :, 0:LANES] = masses
                gather16[unit, :, LANES:] = masses
                square, closing, masses = turned(square), turned(closing), turned(masses)
        return carry

    lax.fori_loop(0, (totals[1] + PREPARED - 1) // PREPARED, prepare, 0)
    for number in range(2):
        source16[UNITS + number] = jnp.zeros((WIDTH, 2 * LANES), BF16)
        gather16[UNITS + number] = jnp.zeros((16, 2 * LANES), F32)
    for number, own in enumerate(own_cells()):
        for half in range(2):
            line = slice(4 * own + 2 * half, 4 * own + 2 * half + 1)
            for field, ref in enumerate((sound, rho, press)):
                spread(mine, 2 * number + half, field, ref[line, :])
    mine[2 * OWN] = jnp.ones((LANES // 8, 3, 8, LANES), F32)
    total_acc[...] = jnp.zeros_like(total_acc)
    for ref in (force0, force1, force2, force3, force4, force5, force6, force7):
        ref[...] = jnp.zeros_like(ref)
    walk = listed(plan)
    distances, forces, collect = force_parts(
        UNROLL, target16, source16, gather16, sound, rho, press, mine, total_acc
    )
    carry = begin(walk, (jnp.int32(0), jnp.int32(0)), distances, (far0, far1, far2, far3, far4, far5, far6, far7))
    last, _ = pipelined(
        walk,
        (totals[0] + TURN - 1) // TURN,
        distances,
        forces,
        collect,
        (far0, far1, far2, far3, far4, far5, far6, far7),
        (force0, force1, force2, force3, force4, force5, force6, force7),
        carry,
    )
    for state, force in zip(last, (force0, force1, force2, force3, force4, force5, force6, force7)):
        collect(walk[1](state), force)
    for number, own in enumerate(own_cells()):
        x, y, z = number // 4, number // 2 % 2, number % 2
        for half in range(2):
            chunk = 2 * number + half
            sums = total_acc[chunk].T + partial_ref[chunk]
            sums = sums[0:4] + sums[4:8] + sums[8:12]
            top = (2 * own + half) * ROWS
            shown = near_ref[top + 3 : top + 4, :] > 0.0
            part = slice(half * LANES, (half + 1) * LANES)
            for axis in range(3):
                offset = float((own // 16, own // 4 % 4, own % 4)[axis] - 2)
                place = near_ref[top + axis : top + axis + 1, :] + offset
                value = (-6.0 * SIGMA) * (sums[axis : axis + 1] - place * sums[3:4])
                out_ref[axis, x, y, z : z + 1, part] = jnp.where(shown, value, 0.0)


def vmem(number):
    return [pl.BlockSpec(memory_space=pltpu.VMEM) for _ in range(number)]


def smem():
    return pl.BlockSpec(memory_space=pltpu.SMEM)


CELL_BLOCK = (2 * ROWS, LANES)
NEAR = (WIDE, WIDE, WIDE)
TARGETS = jax.ShapeDtypeStruct((2 * OWN + 1, LANES, WIDTH), BF16)


def first_call(own):
    return pl.pallas_call(
        first_kernel,
        out_shape=(
            jax.ShapeDtypeStruct(NEAR + CELL_BLOCK, F32),
            jax.ShapeDtypeStruct((2 * OWN, LANES), F32),
            TARGETS,
        ),
        in_specs=vmem(1),
        out_specs=tuple(vmem(3)),
        scratch_shapes=[
            pltpu.VMEM((2 * OWN, WIDTH, LANES), BF16),
            pltpu.VMEM((2 * OWN, LANES), F32),
            pltpu.VMEM((OWN_UNROLL // 2, LANES, 2 * LANES), F32),
            pltpu.VMEM((OWN_UNROLL // 2, LANES, 2 * LANES), F32),
            pltpu.VMEM((OWN_UNROLL // 2, LANES, 2 * LANES), F32),
            pltpu.VMEM((OWN_UNROLL // 2, LANES, 2 * LANES), F32),
            pltpu.VMEM((2 * OWN + 1, LANES, LANES), F32),
        ]
        + exchange_sems(1),
        compiler_params=pltpu.CompilerParams(collective_id=0, has_side_effects=True),
        name="first",
    )(own)


def density_call(near, partial, targets):
    return pl.pallas_call(
        density_kernel,
        out_shape=(
            jax.ShapeDtypeStruct((2, 2, 2, SLOTS), F32),
            jax.ShapeDtypeStruct((2, 2, 2, 2, LANES), F32),
            jax.ShapeDtypeStruct((PLAN,), jnp.int32),
        ),
        in_specs=vmem(3),
        out_specs=tuple(vmem(2) + [smem()]),
        scratch_shapes=[
            pltpu.VMEM((UNITS + 2, WIDTH, LANES), BF16),
            pltpu.VMEM((PADDED, LANES), F32),
            pltpu.VMEM((UNROLL // 2, LANES, 2 * LANES), F32),
            pltpu.VMEM((UNROLL // 2, LANES, 2 * LANES), F32),
            pltpu.VMEM((UNROLL // 2, LANES, 2 * LANES), F32),
            pltpu.VMEM((UNROLL // 2, LANES, 2 * LANES), F32),
            pltpu.VMEM((UNROLL // 2, LANES, 2 * LANES), F32),
            pltpu.VMEM((UNROLL // 2, LANES, 2 * LANES), F32),
            pltpu.VMEM((UNROLL // 2, LANES, 2 * LANES), F32),
            pltpu.VMEM((UNROLL // 2, LANES, 2 * LANES), F32),
            pltpu.VMEM((2 * OWN + 1, LANES, LANES), F32),
        ],
        name="density",
    )(near, partial, targets)


def force_scratch(tiles, padded, unroll, turn):
    block = pltpu.VMEM((unroll, LANES, 2 * LANES), F32)
    return [
        pltpu.VMEM((tiles, WIDTH, 2 * LANES), BF16),
        pltpu.VMEM((tiles, 16, 2 * LANES), F32),
        pltpu.VMEM((padded, LANES), F32),
        pltpu.VMEM((padded, LANES), F32),
        pltpu.VMEM((padded, LANES), F32),
        pltpu.VMEM((2 * OWN + 1, LANES // 8, 3, 8, LANES), F32),
        *[block] * (2 * turn),
        pltpu.VMEM((2 * OWN + 1, LANES, 16), F32),
    ]


def second_call(place, speed, rho):
    return pl.pallas_call(
        second_kernel,
        out_shape=(
            jax.ShapeDtypeStruct(NEAR + CELL_BLOCK, F32),
            jax.ShapeDtypeStruct(NEAR + (2, LANES), F32),
            jax.ShapeDtypeStruct((2 * OWN, 16, LANES), F32),
            TARGETS,
        ),
        in_specs=vmem(3),
        out_specs=tuple(vmem(4)),
        scratch_shapes=force_scratch(2 * OWN, 2 * OWN, OWN_UNROLL, OWN_TURN) + exchange_sems(2),
        compiler_params=pltpu.CompilerParams(collective_id=1, has_side_effects=True),
        name="second",
    )(place, speed, rho)


def force_call(plan, near, speed, rho, partial, targets):
    return pl.pallas_call(
        force_kernel,
        out_shape=jax.ShapeDtypeStruct((3, 2, 2, 2, SLOTS), F32),
        in_specs=[smem()] + vmem(5),
        out_specs=vmem(1)[0],
        scratch_shapes=force_scratch(UNITS + 2, PADDED, UNROLL, TURN),
        name="force",
    )(plan, near, speed, rho, partial, targets)


def per_device(positions, velocities, masses, entropy, counts):
    slot_ids = lax.broadcasted_iota(jnp.int32, masses.shape, 3)
    weight = jnp.where(slot_ids < counts[..., None], masses, 0.0)
    halves = masses.shape[:3] + (2, LANES)

    def blocks(parts):
        joined = jnp.stack([part.reshape(halves) for part in parts], axis=4)
        return joined.reshape(masses.shape[:3] + CELL_BLOCK)

    place = blocks([positions[0], positions[1], positions[2], weight])
    speed = blocks([velocities[0], velocities[1], velocities[2], entropy])
    near, partial, targets = first_call(place)
    near = near.reshape(CELLS * 8, LANES)
    density, own_rho, plan = density_call(near, partial, targets)
    near_speed, near_rho, sums, targets = second_call(place, speed, own_rho)
    near_speed = near_speed.reshape(CELLS * 8, LANES)
    accel = force_call(plan, near, near_speed, near_rho.reshape(TILES, LANES), sums, targets)
    return density, accel


def solution(mesh):
    return jax.shard_map(
        per_device,
        mesh=mesh,
        in_specs=(
            P(None, "gx", "gy", "gz", None),
            P(None, "gx", "gy", "gz", None),
            P("gx", "gy", "gz", None),
            P("gx", "gy", "gz", None),
            P("gx", "gy", "gz"),
        ),
        out_specs=(P("gx", "gy", "gz", None), P(None, "gx", "gy", "gz", None)),
        check_vma=False,
    )
```

```python
import functools
import math

import jax
import jax.numpy as jnp
from jax import lax
from jax.experimental import pallas as pl
from jax.experimental.pallas import tpu as pltpu
from jax.sharding import PartitionSpec as P

SIGMA = 8.0 / math.pi
GAMMA = 5.0 / 3.0
SOFTEN = 0.01
TINY = 1e-12
SLOTS = 256
WIDE = 4
CELLS = WIDE * WIDE * WIDE
OWN = 8
LANES = 128
TILES = 2 * CELLS
UNITS = 2 * TILES
UNROLL = 2
TURN = 8
OWN_UNROLL = 4
OWN_TURN = 4
LIST = 128
ORDER_AT = 9 * LIST
COUNT_AT = ORDER_AT + 24
NEEDED_AT = COUNT_AT + 24
TOTAL_AT = NEEDED_AT + 144
PLAN = 11 * LIST
PREPARED = 4
CHUNK_STEPS = 2 * OWN // OWN_UNROLL
OWN_STEPS = 2 * OWN * CHUNK_STEPS
HALF = LANES // 2
ROWS = 4
GROUPS = 6
WIDTH = 8 * GROUPS
PADDED = UNITS + 8
F32 = jnp.float32
BF16 = jnp.bfloat16


def cell_id(x, y, z):
    return (x * WIDE + y) * WIDE + z


def own_cells():
    return [cell_id(1 + n // 4, 1 + n // 2 % 2, 1 + n % 2) for n in range(OWN)]


def halo_neighbours(number):
    x, y, z = 1 + number // 4, 1 + number // 2 % 2, 1 + number % 2
    around = [
        cell_id(x + dx, y + dy, z + dz)
        for dx in (-1, 0, 1)
        for dy in (-1, 0, 1)
        for dz in (-1, 0, 1)
    ]
    return [other for other in around if other not in own_cells()]


def unit_bits(near_ref):
    lower = near_ref[pl.ds(ROWS - 1, CELLS, stride=2 * ROWS), :]
    upper = near_ref[pl.ds(2 * ROWS - 1, CELLS, stride=2 * ROWS), :]
    ids = lax.broadcasted_iota(jnp.int32, (8, LANES), 0)
    lanes = lax.broadcasted_iota(jnp.int32, (8, LANES), 1)
    power = jnp.ones((8, LANES), F32)
    for bit in range(3):
        power = jnp.where((ids & (1 << bit)) > 0, power * float(4 ** (1 << bit)), power)
    bits = []
    for group in range(CELLS // 8):
        part = slice(8 * group, 8 * group + 8)
        middle = lanes == HALF
        value = jnp.where(middle & (lower[part] > 0.0), power, 0.0)
        value = value + jnp.where((middle | (lanes == 0)) & (upper[part] > 0.0), power, 0.0)
        bits.append(jnp.sum(value).astype(jnp.int32))

    def extra_of(cell):
        return (bits[cell // 8] >> (2 * (cell % 8))) & 3

    return extra_of


class View:
    def __init__(self, plan, base):
        self.plan, self.base = plan, base

    def __getitem__(self, index):
        return self.plan[self.base + index]

    def __setitem__(self, index, value):
        self.plan[self.base + index] = value


def views(plan):
    return [View(plan, base) for base in (0, ORDER_AT, COUNT_AT, NEEDED_AT, TOTAL_AT)]


def build_plan(extra_of, plan):
    tiles, order, count_of, needed, totals = views(plan)
    used = jnp.int32(0)
    for cell in range(CELLS):
        if cell in own_cells():
            continue
        needed[used] = jnp.int32(2 * cell)
        needed[used + 1] = jnp.int32(2 * cell + 1)
        used = used + 1 + (extra_of(cell) >> 1)
    for extra in range(PREPARED - 1):
        needed[used + extra] = jnp.int32(0)
    totals[1] = used
    total = jnp.int32(0)
    place = jnp.int32(0)
    for number, own in enumerate(own_cells()):
        where = jnp.int32(number * LIST)
        for other in halo_neighbours(number):
            for unit in range(4):
                tiles[where + unit] = jnp.int32(4 * other + unit)
            where = where + 1 + extra_of(other)
        for extra in range(2 * UNROLL - 1):
            tiles[where + extra] = jnp.int32(UNITS)
        count = (where - number * LIST + 2 * UNROLL - 1) // (2 * UNROLL)
        for half in range(2):
            order[place] = jnp.int32(2 * number + half)
            count_of[place] = count
            used = 1 if half == 0 else extra_of(own) >> 1
            place = place + used
            total = total + used * count
    order[place] = jnp.int32(2 * OWN)
    count_of[place] = jnp.int32(1 << 20)
    for extra in range(LIST):
        tiles[OWN * LIST + extra] = jnp.int32(UNITS)
    totals[0] = total


def listed(plan):
    tiles, order, count_of, _, _ = views(plan)

    def advance(state):
        place, step = state
        more = step + 1 < count_of[place]
        return jnp.where(more, place, place + 1), jnp.where(more, step + 1, 0)

    def where_is(state):
        chunk = order[state[0]]
        start = (chunk >> 1) * LIST + state[1] * (2 * UNROLL)
        units = [tiles[start + number] for number in range(2 * UNROLL)]
        return chunk, [(units[2 * n], units[2 * n + 1] ^ 1) for n in range(UNROLL)]

    return advance, where_is


def pick(ref, tile):
    if not isinstance(tile, tuple):
        return ref[tile]
    low, high = tile
    lanes = lax.broadcasted_iota(jnp.int32, ref.shape[1:], 1)
    return jnp.where((lanes & HALF) == 0, ref[low], ref[high])


def pick_row(ref, tile):
    if not isinstance(tile, tuple):
        return ref[pl.ds(tile, 1), :]
    low, high = tile
    lanes = lax.broadcasted_iota(jnp.int32, (1, LANES), 1)
    return jnp.where((lanes & HALF) == 0, ref[pl.ds(low, 1), :], ref[pl.ds(high, 1), :])


def turned(value):
    return pltpu.roll(value, HALF, 1)


def put_both(ref, value):
    ref[pl.ds(0, TILES, stride=2), :] = value
    ref[pl.ds(1, TILES, stride=2), :] = turned(value)


def own_walk():
    def advance(state):
        return (jnp.minimum(state[0] + 1, OWN_STEPS - 1),)

    def where_is(state):
        first = (state[0] % CHUNK_STEPS) * OWN_UNROLL
        return state[0] // CHUNK_STEPS, [first + number for number in range(OWN_UNROLL)]

    return advance, where_is


def split(value):
    high = value.astype(BF16).astype(F32)
    rest = value - high
    middle = rest.astype(BF16).astype(F32)
    low = rest - middle
    return high, middle, low


PAIRS = ((0, 0), (0, 1), (1, 0), (1, 1), (0, 2), (2, 0))


def needed_tiles(plan, turn):
    needed = views(plan)[3]
    return [needed[turn * PREPARED + number] for number in range(PREPARED)]


def choose_rows(place, half, speed=None):
    other = pltpu.roll(place, 4, 0)
    row = lax.broadcasted_iota(jnp.int32, (8, LANES), 0)
    place = jnp.where(half > 0, other, place)
    if speed is None:
        return jnp.where(row < 4, place, 0.0)
    return jnp.where(row < 4, place, jnp.where(half > 0, speed, pltpu.roll(speed, 4, 0)))


def tile_rows(place, half, speed=None):
    if half:
        place = pltpu.roll(place, 4, 0)
    elif speed is not None:
        speed = pltpu.roll(speed, 4, 0)
    row = lax.broadcasted_iota(jnp.int32, (8, LANES), 0)
    return jnp.where(row < 4, place, 0.0 if speed is None else speed)


def cell_base(cell):
    row = lax.broadcasted_iota(jnp.int32, (8, LANES), 0)
    x, y, z = [
        (value - 2).astype(F32) for value in (cell >> 4, (cell >> 2) & 3, cell & 3)
    ]
    return jnp.where(row == 0, x, jnp.where(row == 1, y, jnp.where(row == 2, z, 0.0)))


def stack_groups(groups):
    return jnp.concatenate(groups, axis=0)


class Tile:
    def __init__(self, rows, base, moving):
        row = lax.broadcasted_iota(jnp.int32, (8, LANES), 0)
        self.moving = moving
        self.row = row
        self.is_x = row < 3
        self.is_xv = (row < 3) | ((row >= 4) & (row < 7))
        self.weight = jnp.broadcast_to(rows[3:4], (8, LANES))
        self.values = jnp.where((self.weight > 0.0) & self.is_xv, rows + base, 0.0)
        self.pieces = split(self.values)
        squares = self.values * self.values
        self.norm = split(self.fold(squares))
        if moving:
            self.turn = split(4.0 * self.fold(self.values * pltpu.roll(self.values, 4, 0)))

    def fold(self, value):
        total = jnp.sum(jnp.where(self.is_x, value, 0.0), axis=0, keepdims=True)
        return jnp.broadcast_to(total, (8, LANES))

    def place(self, value, third, seventh):
        rest = jnp.where(self.row == 3, third, jnp.where(self.row == 7, seventh, 0.0))
        return jnp.where(self.is_xv, value, rest)

    def target(self):
        groups = []
        for group, (mine, _) in enumerate(PAIRS):
            if group < 3:
                groups.append(self.place(self.pieces[mine], 1.0, self.norm[group]))
            else:
                third = self.turn[group - 3] if self.moving else 0.0
                groups.append(self.place(self.pieces[mine], third, 0.0))
        return stack_groups(groups)

    def square(self):
        groups = []
        scaled = [jnp.where(self.is_x, -2.0 * piece, 0.0) for piece in self.pieces]
        for group, (_, theirs) in enumerate(PAIRS):
            if group < 3:
                groups.append(self.place(scaled[theirs], self.norm[group], 1.0))
            else:
                groups.append(scaled[theirs])
        return stack_groups(groups)

    def closing(self):
        groups = []
        scaled = [-4.0 * pltpu.roll(piece, 4, 0) for piece in self.pieces]
        for group, (_, theirs) in enumerate(PAIRS):
            third = self.turn[group] if group < 3 else 1.0
            groups.append(self.place(scaled[theirs], third, 0.0))
        return stack_groups(groups)

    def gather(self):
        moments = jnp.where(self.is_x, self.values * self.weight, 0.0)
        moments = jnp.where(self.row == 3, self.weight, moments)
        high, middle, low = split(moments)
        first = jnp.where(self.row < 4, high, pltpu.roll(middle, 4, 0))
        return stack_groups([first, jnp.where(self.row < 4, low, 0.0)])


def pipelined(walk, pairs, distances, work, collect, far, kept, carry):
    advance, where_is = walk

    def turn(_, carry):
        last, now = carry
        after = following(advance, advance(now[-1]), len(far))
        ahead = [distances(where_is(state)) for state in after]
        for state, force in zip(last, kept):
            collect(where_is(state), force)
        for state, block, force in zip(now, far, kept):
            work(where_is(state), block, force)
        for block, values in zip(far, ahead):
            store_all(block, values)
        return now, after

    return lax.fori_loop(0, pairs, turn, carry)


def store_all(block, values):
    for number, value in enumerate(values):
        block[number] = value


def following(advance, state, count):
    states = [state]
    while len(states) < count:
        states.append(advance(states[-1]))
    return tuple(states)


def begin(walk, state, distances, far):
    advance, where_is = walk
    now = following(advance, state, len(far))
    for block, step in zip(far, now):
        store_all(block, distances(where_is(step)))
    return now, now


def density_parts(unroll, target16, source16, weights, total_acc):
    def distances(step):
        chunk, ids = step
        mine = target16[chunk]
        return [
            jnp.dot(
                mine,
                jnp.concatenate([pick(source16, ids[2 * pair]), pick(source16, ids[2 * pair + 1])], axis=1),
                preferred_element_type=F32,
            )
            for pair in range(unroll // 2)
        ]

    def add(step, far, _):
        chunk, ids = step
        mass = [pick_row(weights, tile) for tile in ids]
        for group in range(LANES // 8):
            rows = slice(group * 8, group * 8 + 8)
            acc = total_acc[chunk, rows, :]
            for number in range(unroll):
                lanes = slice((number % 2) * LANES, (number % 2 + 1) * LANES)
                square = jnp.maximum(far[number // 2, rows, lanes], TINY)
                radius = square * lax.rsqrt(square)
                rest = 1.0 - radius
                near = 0.5 - 3.0 * (square * rest)
                clipped = jnp.maximum(rest, 0.0)
                value = jnp.minimum(near, clipped * clipped * clipped)
                acc = acc + value * mass[number]
            total_acc[chunk, rows, :] = acc

    def collect(step, kept):
        pass

    return distances, add, collect


def density_rows(total_acc, chunk):
    return (2.0 * SIGMA) * jnp.sum(total_acc[chunk].T, axis=0, keepdims=True)


def force_parts(unroll, target16, source16, gather16, sound, rho, press, mine, total_acc):
    def distances(step):
        chunk, ids = step
        return [
            jnp.dot(target16[chunk], pick(source16, tile), preferred_element_type=F32)
            for tile in ids
        ]

    def forces(step, far, force):
        chunk, ids = step
        sound_j = [pick_row(sound, tile) for tile in ids]
        rho_j = [pick_row(rho, tile) for tile in ids]
        press_j = [pick_row(press, tile) for tile in ids]
        for group in range(LANES // 16):
            for number in range(unroll):
                parts = []
                for sub in range(2):
                    rows = slice(group * 16 + sub * 8, group * 16 + sub * 8 + 8)
                    square = jnp.minimum(jnp.maximum(far[number, rows, 0:LANES], TINY), 1.0)
                    closing = jnp.minimum(far[number, rows, LANES:], 0.0)
                    inverse = lax.rsqrt(square)
                    radius = square * inverse
                    slope = jnp.maximum(
                        4.0 - 3.0 * radius, jnp.minimum(inverse + radius, 2.5)
                    )
                    slope = slope - 2.0
                    approach = closing / (square + SOFTEN)
                    both_rho = mine[chunk, group * 2 + sub, 1] + rho_j[number]
                    both_sound = mine[chunk, group * 2 + sub, 0] + sound_j[number]
                    both_press = mine[chunk, group * 2 + sub, 2] + press_j[number]
                    viscous = approach * (approach - both_sound) / both_rho
                    parts.append((both_press + viscous) * slope)
                value = jnp.concatenate(parts, axis=0)
                rows = slice(group * 16, group * 16 + 16)
                force[number, rows, 0:LANES] = value
                force[number, rows, LANES:] = value - value.astype(BF16).astype(F32)

    def collect(step, force):
        chunk, ids = step
        acc = None
        for number, tile in enumerate(ids):
            part = lax.dot_general(
                force[number],
                pick(gather16, tile),
                (((1,), (1,)), ((), ())),
                preferred_element_type=F32,
            )
            acc = part if acc is None else acc + part
        total_acc[chunk] += acc

    return distances, forces, collect


def states_of(weight, density, entropy):
    active = weight > 0.0
    safe = jnp.where(active, density, 1.0)
    entropy = jnp.where(active, entropy, 1.0)
    root = jnp.exp(jnp.log(safe) * (1.0 / 3.0))
    return jnp.sqrt(GAMMA * entropy) * root, 4.0 * safe, entropy / root


def spread(ref, chunk, field, line):
    wide = jnp.broadcast_to(line, (LANES, LANES)).T
    for group in range(LANES // 8):
        ref[chunk, group, field] = wide[group * 8 : group * 8 + 8]


class Exchange:
    def __init__(self, arrays, local_sem, send_sem, recv_sem):
        self.arrays = arrays
        self.send_sem, self.recv_sem = send_sem, recv_sem
        self.local = [
            pltpu.make_async_copy(own, near.at[1:3, 1:3, 1:3], local_sem.at[number])
            for number, (own, near) in enumerate(arrays)
        ]
        self.moved = {
            axis: {
                0: lax.axis_index(axis),
                1: lax.rem(lax.axis_index(axis) + 1, lax.axis_size(axis)),
                -1: lax.rem(lax.axis_index(axis) + lax.axis_size(axis) - 1, lax.axis_size(axis)),
            }
            for axis in ("gx", "gy", "gz")
        }
        self.plane = [(dy, dz) for dz in (-1, 1) for dy in (-1, 0, 1)] + [(-1, 0), (1, 0)]
        self.count = 0

    def device(self, dx, dy, dz):
        return {
            "gx": self.moved["gx"][dx],
            "gy": self.moved["gy"][dy],
            "gz": self.moved["gz"][dz],
        }

    def greet(self):
        barrier = pltpu.get_barrier_semaphore()
        others = [(0, dy, dz) for dy, dz in self.plane] + [(-1, 0, 0), (1, 0, 0)]
        for other in others:
            pl.semaphore_signal(
                barrier,
                inc=1,
                device_id=self.device(*other),
                device_id_type=pl.DeviceIdType.MESH,
            )
        for copy in self.local:
            copy.start()

    def send(self, source, dest, other):
        copy = pltpu.make_async_remote_copy(
            src_ref=source,
            dst_ref=dest,
            send_sem=self.send_sem.at[self.count],
            recv_sem=self.recv_sem.at[self.count],
            device_id=self.device(*other),
            device_id_type=pl.DeviceIdType.MESH,
        )
        self.count += 1
        copy.start()
        return copy

    def start_plane(self):
        pl.semaphore_wait(pltpu.get_barrier_semaphore(), len(self.plane) + 2)
        taken = {-1: slice(0, 1), 0: slice(0, 2), 1: slice(1, 2)}
        landed = {-1: slice(3, 4), 0: slice(1, 3), 1: slice(0, 1)}
        self.copies = [
            self.send(
                own.at[:, taken[dy], taken[dz]], near.at[1:3, landed[dy], landed[dz]], (0, dy, dz)
            )
            for own, near in self.arrays
            for dy, dz in self.plane
        ]

    def start_gx(self):
        for copy in self.local + self.copies:
            copy.wait()
        self.copies = []
        for _, near in self.arrays:
            self.copies.append(self.send(near.at[2:3], near.at[0:1], (1, 0, 0)))
            self.copies.append(self.send(near.at[1:2], near.at[3:4], (-1, 0, 0)))

    def finish(self):
        for copy in self.copies:
            copy.wait()


def exchange_sems(arrays):
    return [
        pltpu.SemaphoreType.DMA((arrays,)),
        pltpu.SemaphoreType.DMA((10 * arrays,)),
        pltpu.SemaphoreType.DMA((10 * arrays,)),
    ]


def staged(walk, parts, distances, work, collect, far, kept, exchange):
    carry = begin(walk, (jnp.int32(0),), distances, far)
    stages = (exchange.start_plane, exchange.start_gx, exchange.finish)[-len(parts) :]
    for stage, pairs in zip(stages, parts):
        carry = pipelined(walk, pairs, distances, work, collect, far, kept, carry)
        stage()
    return carry[0]


DENSITY_PARTS = (15, 1)
FORCE_PARTS = (3, 10, 3)


def own_cell_rows(ref, number):
    return ref[number // 4, number // 2 % 2, number % 2]


def first_kernel(own_ref, near_ref, partial_ref, target16, source16, weights, far0, far1, far2, far3, total_acc, local_sem, send_sem, recv_sem):
    exchange = Exchange([(own_ref, near_ref)], local_sem, send_sem, recv_sem)
    exchange.greet()
    exchange.start_plane()
    for number, own in enumerate(own_cells()):
        base = cell_base(jnp.int32(own))
        rows = own_cell_rows(own_ref, number)
        for half in range(2):
            chunk = 2 * number + half
            tile = Tile(tile_rows(rows, half), base, False)
            target16[chunk] = tile.target().T.astype(BF16)
            source16[chunk] = tile.square().astype(BF16)
            weights[chunk : chunk + 1, :] = tile.weight[0:1]
    target16[2 * OWN] = jnp.zeros((LANES, WIDTH), BF16)
    total_acc[...] = jnp.zeros_like(total_acc)
    parts = density_parts(OWN_UNROLL, target16, source16, weights, total_acc)
    staged(own_walk(), DENSITY_PARTS, *parts, (far0, far1, far2, far3), (None,) * OWN_TURN, exchange)
    for chunk in range(2 * OWN):
        partial_ref[chunk : chunk + 1, :] = density_rows(total_acc, chunk)


def density_kernel(near_ref, partial_ref, target16, out_ref, own_ref, plan, source16, weights, far0, far1, far2, far3, far4, far5, far6, far7, total_acc):
    build_plan(unit_bits(near_ref), plan)
    totals = views(plan)[4]
    put_both(weights, near_ref[pl.ds(3, TILES, stride=ROWS), :])
    weights[UNITS:PADDED, :] = jnp.zeros((8, LANES), F32)

    def prepare(turn, carry):
        for tile in needed_tiles(plan, turn):
            cell = tile >> 1
            rows = near_ref[pl.ds(pl.multiple_of(cell * 8, 8), 8), :]
            square = Tile(choose_rows(rows, tile & 1), cell_base(cell), False).square()
            source16[2 * tile] = square.astype(BF16)
            source16[2 * tile + 1] = turned(square).astype(BF16)
        return carry

    lax.fori_loop(0, (totals[1] + PREPARED - 1) // PREPARED, prepare, 0)
    for number in range(2):
        source16[UNITS + number] = jnp.zeros((WIDTH, LANES), BF16)
    total_acc[...] = jnp.zeros_like(total_acc)
    walk = listed(plan)
    distances, add, collect = density_parts(UNROLL, target16, source16, weights, total_acc)
    carry = begin(walk, (jnp.int32(0), jnp.int32(0)), distances, (far0, far1, far2, far3, far4, far5, far6, far7))
    pipelined(
        walk, (totals[0] + TURN - 1) // TURN, distances, add, collect, (far0, far1, far2, far3, far4, far5, far6, far7), (None,) * TURN, carry
    )
    for number, own in enumerate(own_cells()):
        x, y, z = number // 4, number // 2 % 2, number % 2
        for half in range(2):
            chunk = 2 * number + half
            part = slice(half * LANES, (half + 1) * LANES)
            row = (2 * own + half) * ROWS + 3
            value = partial_ref[chunk : chunk + 1, :] + density_rows(total_acc, chunk)
            value = jnp.where(near_ref[row : row + 1, :] > 0.0, value, 0.0)
            out_ref[x, y, z : z + 1, part] = value
            own_ref[x, y, z, half : half + 1, :] = value


def second_kernel(place_ref, speed_ref, rho_ref, near_speed_ref, near_rho_ref, partial_ref, target16, source16, gather16, sound, rho, press, mine, far0, far1, far2, far3, force0, force1, force2, force3, total_acc, local_sem, send_sem, recv_sem):
    exchange = Exchange(
        [(speed_ref, near_speed_ref), (rho_ref, near_rho_ref)], local_sem, send_sem, recv_sem
    )
    exchange.greet()
    for number, own in enumerate(own_cells()):
        base = cell_base(jnp.int32(own))
        places = own_cell_rows(place_ref, number)
        speeds = own_cell_rows(speed_ref, number)
        density = own_cell_rows(rho_ref, number)
        for half in range(2):
            chunk = 2 * number + half
            rows = tile_rows(places, half, speeds)
            tile = Tile(rows, base, True)
            target16[chunk] = tile.target().T.astype(BF16)
            source16[chunk, :, 0:LANES] = tile.square().astype(BF16)
            source16[chunk, :, LANES:] = tile.closing().astype(BF16)
            masses = tile.gather()
            gather16[chunk, :, 0:LANES] = masses
            gather16[chunk, :, LANES:] = masses
            states = states_of(rows[3:4], density[half : half + 1], rows[7:8])
            for field, (value, far) in enumerate(zip(states, (sound, rho, press))):
                far[chunk : chunk + 1, :] = value
                spread(mine, chunk, field, value)
    target16[2 * OWN] = jnp.zeros((LANES, WIDTH), BF16)
    total_acc[...] = jnp.zeros_like(total_acc)
    for ref in (force0, force1, force2, force3):
        ref[...] = jnp.zeros_like(ref)
    parts = force_parts(
        OWN_UNROLL, target16, source16, gather16, sound, rho, press, mine, total_acc
    )
    walk = own_walk()
    last = staged(walk, FORCE_PARTS, *parts, (far0, far1, far2, far3), (force0, force1, force2, force3), exchange)
    for state, force in zip(last, (force0, force1, force2, force3)):
        parts[2](walk[1](state), force)
    for chunk in range(2 * OWN):
        partial_ref[chunk] = total_acc[chunk].T


def force_kernel(plan, near_ref, speed_ref, rho_ref, partial_ref, target16, out_ref, source16, gather16, sound, rho, press, mine, far0, far1, far2, far3, far4, far5, far6, far7, force0, force1, force2, force3, force4, force5, force6, force7, total_acc):
    totals = views(plan)[4]
    states = states_of(
        near_ref[pl.ds(3, TILES, stride=ROWS), :],
        rho_ref[...],
        speed_ref[pl.ds(3, TILES, stride=ROWS), :],
    )
    for value, ref in zip(states, (sound, rho, press)):
        put_both(ref, value)
        ref[UNITS:PADDED, :] = jnp.ones((8, LANES), F32)

    def prepare(turn, carry):
        for number in needed_tiles(plan, turn):
            cell = number >> 1
            place = pl.ds(pl.multiple_of(cell * 8, 8), 8)
            rows = choose_rows(near_ref[place, :], number & 1, speed_ref[place, :])
            tile = Tile(rows, cell_base(cell), True)
            square, closing, masses = tile.square(), tile.closing(), tile.gather()
            for unit in (2 * number, 2 * number + 1):
                source16[unit, :, 0:LANES] = square.astype(BF16)
                source16[unit, :, LANES:] = closing.astype(BF16)
                gather16[unit, :, 0:LANES] = masses
                gather16[unit, :, LANES:] = masses
                square, closing, masses = turned(square), turned(closing), turned(masses)
        return carry

    lax.fori_loop(0, (totals[1] + PREPARED - 1) // PREPARED, prepare, 0)
    for number in range(2):
        source16[UNITS + number] = jnp.zeros((WIDTH, 2 * LANES), BF16)
        gather16[UNITS + number] = jnp.zeros((16, 2 * LANES), F32)
    for number, own in enumerate(own_cells()):
        for half in range(2):
            line = slice(4 * own + 2 * half, 4 * own + 2 * half + 1)
            for field, ref in enumerate((sound, rho, press)):
                spread(mine, 2 * number + half, field, ref[line, :])
    mine[2 * OWN] = jnp.ones((LANES // 8, 3, 8, LANES), F32)
    total_acc[...] = jnp.zeros_like(total_acc)
    for ref in (force0, force1, force2, force3, force4, force5, force6, force7):
        ref[...] = jnp.zeros_like(ref)
    walk = listed(plan)
    distances, forces, collect = force_parts(
        UNROLL, target16, source16, gather16, sound, rho, press, mine, total_acc
    )
    carry = begin(walk, (jnp.int32(0), jnp.int32(0)), distances, (far0, far1, far2, far3, far4, far5, far6, far7))
    last, _ = pipelined(
        walk,
        (totals[0] + TURN - 1) // TURN,
        distances,
        forces,
        collect,
        (far0, far1, far2, far3, far4, far5, far6, far7),
        (force0, force1, force2, force3, force4, force5, force6, force7),
        carry,
    )
    for state, force in zip(last, (force0, force1, force2, force3, force4, force5, force6, force7)):
        collect(walk[1](state), force)
    for number, own in enumerate(own_cells()):
        x, y, z = number // 4, number // 2 % 2, number % 2
        for half in range(2):
            chunk = 2 * number + half
            sums = total_acc[chunk].T + partial_ref[chunk]
            sums = sums[0:4] + sums[4:8] + sums[8:12]
            top = (2 * own + half) * ROWS
            shown = near_ref[top + 3 : top + 4, :] > 0.0
            part = slice(half * LANES, (half + 1) * LANES)
            for axis in range(3):
                offset = float((own // 16, own // 4 % 4, own % 4)[axis] - 2)
                place = near_ref[top + axis : top + axis + 1, :] + offset
                value = (-6.0 * SIGMA) * (sums[axis : axis + 1] - place * sums[3:4])
                out_ref[axis, x, y, z : z + 1, part] = jnp.where(shown, value, 0.0)


def vmem(number):
    return [pl.BlockSpec(memory_space=pltpu.VMEM) for _ in range(number)]


def smem():
    return pl.BlockSpec(memory_space=pltpu.SMEM)


CELL_BLOCK = (2 * ROWS, LANES)
NEAR = (WIDE, WIDE, WIDE)
TARGETS = jax.ShapeDtypeStruct((2 * OWN + 1, LANES, WIDTH), BF16)


def first_call(own):
    return pl.pallas_call(
        first_kernel,
        out_shape=(
            jax.ShapeDtypeStruct(NEAR + CELL_BLOCK, F32),
            jax.ShapeDtypeStruct((2 * OWN, LANES), F32),
            TARGETS,
        ),
        in_specs=vmem(1),
        out_specs=tuple(vmem(3)),
        scratch_shapes=[
            pltpu.VMEM((2 * OWN, WIDTH, LANES), BF16),
            pltpu.VMEM((2 * OWN, LANES), F32),
            pltpu.VMEM((OWN_UNROLL // 2, LANES, 2 * LANES), F32),
            pltpu.VMEM((OWN_UNROLL // 2, LANES, 2 * LANES), F32),
            pltpu.VMEM((OWN_UNROLL // 2, LANES, 2 * LANES), F32),
            pltpu.VMEM((OWN_UNROLL // 2, LANES, 2 * LANES), F32),
            pltpu.VMEM((2 * OWN + 1, LANES, LANES), F32),
        ]
        + exchange_sems(1),
        compiler_params=pltpu.CompilerParams(collective_id=0, has_side_effects=True),
        name="first",
    )(own)


def density_call(near, partial, targets):
    return pl.pallas_call(
        density_kernel,
        out_shape=(
            jax.ShapeDtypeStruct((2, 2, 2, SLOTS), F32),
            jax.ShapeDtypeStruct((2, 2, 2, 2, LANES), F32),
            jax.ShapeDtypeStruct((PLAN,), jnp.int32),
        ),
        in_specs=vmem(3),
        out_specs=tuple(vmem(2) + [smem()]),
        scratch_shapes=[
            pltpu.VMEM((UNITS + 2, WIDTH, LANES), BF16),
            pltpu.VMEM((PADDED, LANES), F32),
            pltpu.VMEM((UNROLL // 2, LANES, 2 * LANES), F32),
            pltpu.VMEM((UNROLL // 2, LANES, 2 * LANES), F32),
            pltpu.VMEM((UNROLL // 2, LANES, 2 * LANES), F32),
            pltpu.VMEM((UNROLL // 2, LANES, 2 * LANES), F32),
            pltpu.VMEM((UNROLL // 2, LANES, 2 * LANES), F32),
            pltpu.VMEM((UNROLL // 2, LANES, 2 * LANES), F32),
            pltpu.VMEM((UNROLL // 2, LANES, 2 * LANES), F32),
            pltpu.VMEM((UNROLL // 2, LANES, 2 * LANES), F32),
            pltpu.VMEM((2 * OWN + 1, LANES, LANES), F32),
        ],
        name="density",
    )(near, partial, targets)


def force_scratch(tiles, padded, unroll, turn):
    block = pltpu.VMEM((unroll, LANES, 2 * LANES), F32)
    return [
        pltpu.VMEM((tiles, WIDTH, 2 * LANES), BF16),
        pltpu.VMEM((tiles, 16, 2 * LANES), F32),
        pltpu.VMEM((padded, LANES), F32),
        pltpu.VMEM((padded, LANES), F32),
        pltpu.VMEM((padded, LANES), F32),
        pltpu.VMEM((2 * OWN + 1, LANES // 8, 3, 8, LANES), F32),
        *[block] * (2 * turn),
        pltpu.VMEM((2 * OWN + 1, LANES, 16), F32),
    ]


def second_call(place, speed, rho):
    return pl.pallas_call(
        second_kernel,
        out_shape=(
            jax.ShapeDtypeStruct(NEAR + CELL_BLOCK, F32),
            jax.ShapeDtypeStruct(NEAR + (2, LANES), F32),
            jax.ShapeDtypeStruct((2 * OWN, 16, LANES), F32),
            TARGETS,
        ),
        in_specs=vmem(3),
        out_specs=tuple(vmem(4)),
        scratch_shapes=force_scratch(2 * OWN, 2 * OWN, OWN_UNROLL, OWN_TURN) + exchange_sems(2),
        compiler_params=pltpu.CompilerParams(collective_id=1, has_side_effects=True),
        name="second",
    )(place, speed, rho)


def force_call(plan, near, speed, rho, partial, targets):
    return pl.pallas_call(
        force_kernel,
        out_shape=jax.ShapeDtypeStruct((3, 2, 2, 2, SLOTS), F32),
        in_specs=[smem()] + vmem(5),
        out_specs=vmem(1)[0],
        scratch_shapes=force_scratch(UNITS + 2, PADDED, UNROLL, TURN),
        name="force",
    )(plan, near, speed, rho, partial, targets)


def per_device(positions, velocities, masses, entropy, counts):
    slot_ids = lax.broadcasted_iota(jnp.int32, masses.shape, 3)
    weight = jnp.where(slot_ids < counts[..., None], masses, 0.0)
    halves = masses.shape[:3] + (2, LANES)

    def blocks(parts):
        joined = jnp.stack([part.reshape(halves) for part in parts], axis=4)
        return joined.reshape(masses.shape[:3] + CELL_BLOCK)

    place = blocks([positions[0], positions[1], positions[2], weight])
    speed = blocks([velocities[0], velocities[1], velocities[2], entropy])
    near, partial, targets = first_call(place)
    near = near.reshape(CELLS * 8, LANES)
    density, own_rho, plan = density_call(near, partial, targets)
    near_speed, near_rho, sums, targets = second_call(place, speed, own_rho)
    near_speed = near_speed.reshape(CELLS * 8, LANES)
    accel = force_call(plan, near, near_speed, near_rho.reshape(TILES, LANES), sums, targets)
    return density, accel


def solution(mesh):
    return jax.shard_map(
        per_device,
        mesh=mesh,
        in_specs=(
            P(None, "gx", "gy", "gz", None),
            P(None, "gx", "gy", "gz", None),
            P("gx", "gy", "gz", None),
            P("gx", "gy", "gz", None),
            P("gx", "gy", "gz"),
        ),
        out_specs=(P("gx", "gy", "gz", None), P(None, "gx", "gy", "gz", None)),
        check_vma=False,
    )
```
